32 devices in a mesh: rep: 2 (over z, core), dp: 16 (over x, y).
Axes of the slice: x: 4, y: 4, z: 1, core: 2. Of those that a mesh axis runs over, the one named last changes fastest.
The devices are a block of a 4x4x8 slice.
Arguments:
- x: bfloat16 [32, 1024, 512], P(('rep', 'dp')), parts along dimension 0
- dy: bfloat16 [32, 1024, 512], P(('rep', 'dp')), parts along dimension 0
- w_gate: bfloat16 [2, 512, 8192], P(None, 'dp')
- w_up: bfloat16 [2, 512, 8192], P(None, 'dp')
- w_down: bfloat16 [2, 8192, 512], P(None, 'dp')
- m_w_gate: float32 [2, 512, 8192], P(None, 'dp')
- m_w_up: float32 [2, 512, 8192], P(None, 'dp')
- m_w_down: float32 [2, 8192, 512], P(None, 'dp')
- v_w_gate: float32 [2, 512, 8192], P(None, 'dp')
- v_w_up: float32 [2, 512, 8192], P(None, 'dp')
- v_w_down: float32 [2, 8192, 512], P(None, 'dp')
Outputs:
- output 1: bfloat16 [4, 512, 8192], P('rep', 'dp'), parts along dimension 0
- output 2: bfloat16 [4, 512, 8192], P('rep', 'dp'), parts along dimension 0
- output 3: bfloat16 [4, 8192, 512], P('rep', 'dp'), parts along dimension 0
- output 4: float32 [4, 512, 8192], P('rep', 'dp'), parts along dimension 0
- output 5: float32 [4, 512, 8192], P('rep', 'dp'), parts along dimension 0
- output 6: float32 [4, 8192, 512], P('rep', 'dp'), parts along dimension 0
- output 7: float32 [4, 512, 8192], P('rep', 'dp'), parts along dimension 0
- output 8: float32 [4, 512, 8192], P('rep', 'dp'), parts along dimension 0
- output 9: float32 [4, 8192, 512], P('rep', 'dp'), parts along dimension 0
There are 2 independent parts. The reference program is written for one: setup_inputs(seed, part) draws one part's arguments, and reference() takes and returns one part's arrays. A program takes and returns all parts, laid end to end along the dimension named above; an argument that names none is the same for every part.
All inputs are finite; a program needn't handle non-finite values.
Results may differ from the reference program's by a relative error of at most 0.022.
Values are sent between devices in bfloat16 or wider.
A program may use at most 768 MiB of HBM per device.

```python
import jax
import jax.numpy as jnp
from jax import lax

SEQUENCES = 16
TOKENS = 1024
D = 512
FF = 8192
LAYERS = 2
NAMES = ("w_gate", "w_up", "w_down")
SHAPES = {"w_gate": (LAYERS, D, FF), "w_up": (LAYERS, D, FF), "w_down": (LAYERS, FF, D)}


def bump(key, n, height):
    away = (jnp.arange(n, dtype=jnp.int32) - jax.random.randint(key, (), 0, n, jnp.int32)) % n
    return jnp.where(away < n // 8, height, 1.0)


def together(key, own, strength):
    shared = jax.random.normal(key, own.shape[1:], jnp.float32)
    return (own + strength * shared) * lax.rsqrt(1 + strength * strength)


def setup_inputs(seed: int = 0, part: int = 0) -> dict:
    kx, kdy, ka, kb, kz, kf, kh, kl, *keys = jax.random.split(jax.random.key(seed), 8 + 3 * len(NAMES))
    kx, kdy, ka, kb = (jax.random.fold_in(k, part) for k in (kx, kdy, ka, kb))
    kw, km, kv = (keys[i::3] for i in range(3))
    shape = (SEQUENCES, TOKENS, D)
    much_x, much_dy = jax.random.uniform(kz, (2,), jnp.float32, 0.0, 1.0)
    loud = 2.0 ** jax.random.uniform(jax.random.fold_in(kz, 1), (), jnp.float32, -1.0, 2.0)
    layers = 2.0 ** jax.random.uniform(kl, (LAYERS, 1, 1), jnp.float32, -1.0, 1.0)
    x = together(ka, jax.random.normal(kx, shape, jnp.float32), much_x) * bump(kf, D, 4.0)
    dy = together(kb, jax.random.normal(kdy, shape, jnp.float32), much_dy)
    drawn = {"x": x.astype(jnp.bfloat16), "dy": (loud * dy * (SEQUENCES * TOKENS) ** -0.5).astype(jnp.bfloat16)}
    for key, name in zip(kw, NAMES, strict=True):
        w = jax.random.normal(key, SHAPES[name], jnp.float32) * SHAPES[name][1] ** -0.5
        drawn[name] = (w * {"w_gate": 1.0, "w_up": bump(kh, FF, 4.0), "w_down": layers}[name]).astype(jnp.bfloat16)
    for key, name in zip(km, NAMES, strict=True):
        drawn[f"m_{name}"] = 0.1 * jax.random.normal(key, SHAPES[name], jnp.float32)
    for key, name in zip(kv, NAMES, strict=True):
        drawn[f"v_{name}"] = jax.random.uniform(key, SHAPES[name], jnp.float32, 0.005, 0.015)
    return drawn


def matmul(a, w):
    return jnp.dot(a, w, preferred_element_type=jnp.float32).astype(jnp.bfloat16)


def normed(h):
    wide = h.astype(jnp.float32)
    scale = lax.rsqrt(jnp.mean(wide**2, -1, keepdims=True) + 1e-6)
    return (wide * scale).astype(jnp.bfloat16)


def layer(h, w):
    a = normed(h)
    gate = jnp.dot(a, w["w_gate"], preferred_element_type=jnp.float32)
    up = jnp.dot(a, w["w_up"], preferred_element_type=jnp.float32)
    return h + matmul((jax.nn.silu(gate) * up).astype(jnp.bfloat16), w["w_down"])


def adamw(w, m, v, g):
    m = 0.9 * m + 0.1 * g
    v = 0.95 * v + 0.05 * g * g
    step = m * lax.rsqrt(v + 1e-8) + 0.1 * w
    return (w - 0.02 * step).astype(jnp.bfloat16), m, v


def clipped(gradients, sum_of_squares, count):
    factor = jnp.minimum(1.0, 0.5 * lax.rsqrt(sum_of_squares / count + 1e-30))
    return [g * factor for g in gradients]


def stack(weights, h):
    return lax.scan(lambda h, w: (layer(h, w), None), h, weights)[0]


def reference(x, dy, w_gate, w_up, w_down, m_w_gate, m_w_up, m_w_down, v_w_gate, v_w_up, v_w_down):
    weights = dict(zip(NAMES, (w_gate, w_up, w_down), strict=True))

    def take(so_far, sequence):
        h, by_y = sequence
        _, back = jax.vjp(lambda w: stack(w, h), weights)
        return jax.tree.map(lambda total, term: total + term.astype(jnp.float32), so_far, back(by_y)[0]), None

    none_yet = {name: jnp.zeros(w.shape, jnp.float32) for name, w in weights.items()}
    by_weights, _ = lax.scan(take, none_yet, (x, dy))
    gradients = [by_weights[name].astype(jnp.bfloat16).astype(jnp.float32) for name in NAMES]
    gradients = clipped(gradients, sum(jnp.sum(g * g) for g in gradients), sum(g.size for g in gradients))
    new = [
        adamw(w.astype(jnp.float32), m, v, g)
        for w, m, v, g in zip((w_gate, w_up, w_down), (m_w_gate, m_w_up, m_w_down), (v_w_gate, v_w_up, v_w_down), gradients, strict=True)
    ]
    return tuple(one[which] for which in range(3) for one in new)
```

```python
import functools
import math

import jax
import jax.numpy as jnp
from jax import lax
from jax.experimental import pallas as pl
from jax.experimental.pallas import tpu as pltpu
from jax.sharding import PartitionSpec as P

MESH = pl.DeviceIdType.MESH
BF, F32 = jnp.bfloat16, jnp.float32
LANES = 128
TILE = 512
VMEM_LIMIT = 66_000_000


def dot(a, b, over=(1, 0)):
    return lax.dot_general(a, b, (((over[0],), (over[1],)), ((), ())), preferred_element_type=F32)


def scale_of(wide):
    return lax.rsqrt(jnp.mean(wide**2, -1, keepdims=True) + 1e-6)


def adamw(w, m, v, g):
    m = 0.9 * m + 0.1 * g
    v = 0.95 * v + 0.05 * g * g
    step = m * lax.rsqrt(v + 1e-8) + 0.1 * w
    return (w - 0.02 * step).astype(BF), m, v


def clipped(gradients, sum_of_squares, count):
    factor = jnp.minimum(1.0, 0.5 * lax.rsqrt(sum_of_squares / count + 1e-30))
    return [g * factor for g in gradients]


class Torus:
    def __init__(self, n):
        me = lax.axis_index("dp")
        self.n = n
        self.at = (lax.div(me, n), lax.rem(me, n))

    def step(self, axis, by):
        return lax.rem(self.at[axis] + (by + self.n), self.n)

    def device(self, axis, by):
        x, y = self.at
        moved = self.step(axis, by)
        return {"dp": moved * self.n + y if axis == 0 else x * self.n + moved}


def greet(others):
    barrier = pltpu.get_barrier_semaphore()
    for other in others:
        pl.semaphore_signal(barrier, inc=1, device_id=other, device_id_type=MESH)
    pl.semaphore_wait(barrier, len(others))


def gather_kernel(layers, n, gu_in, d_in, gu_out, d_out, send, recv, push, pull, own):
    torus = Torus(n)
    rep = lax.axis_index("rep")
    core = lax.rem(rep, 2)
    partner = {"rep": rep + 1 - 2 * core}
    lanes, rows = gu_in.shape[-1] // 2, d_in.shape[-2]
    parts = {"all": (0, 1), "a": (0, 2), "b": (1, 2)}

    def place(k, i, j):
        first, second = torus.step(k, i), torus.step(1 - k, j)
        return (first, second) if k == 0 else (second, first)

    def refs(layer, k, block, part, mine=False, whose=core):
        which, of = parts[part]
        wide, high = lanes // of, rows // of
        cols = pl.ds(k * lanes + which * wide, wide)
        tall = pl.ds(which * high, high)
        if mine:
            return gu_in.at[layer, :, whose, :, cols], d_in.at[layer, 2 * whose + k, tall]
        x, y = block
        return gu_out.at[layer, :, x, y, whose, :, cols], d_out.at[layer, 2 * whose + k, x, y, tall]

    greet([torus.device(a, b) for a in (0, 1) for b in (1, -1)] + [partner])

    owns = []
    for layer in range(layers):
        x, y = torus.at
        owns.append(pltpu.make_async_copy(gu_in.at[layer], gu_out.at[layer, :, x, y], own.at[layer, 0]))
        owns.append(pltpu.make_async_copy(d_in.at[layer], d_out.at[layer, :, x, y], own.at[layer, 1]))
    sent = []

    def message(layer, k, group, kind, block, mine=False):
        axis = k if group == 0 else 1 - k
        part = ("all", "all", "a", "b")[kind]
        target = torus.device(axis, (1, -1)[kind % 2])
        there = refs(layer, k, block, part)
        here = refs(layer, k, block, part, mine)
        return [
            pltpu.make_async_remote_copy(s, t, send.at[layer, k, group, kind, i], recv.at[layer, k, group, kind, i], device_id=target, device_id_type=MESH)
            for i, (s, t) in enumerate(zip(here, there, strict=True))
        ]

    def out(layer, k, group, kind, block, mine=False):
        for copy in message(layer, k, group, kind, block, mine):
            copy.start()
            sent.append(copy)

    def arrived(layer, k, group, kind, block):
        for copy in message(layer, k, group, kind, block):
            copy.wait_recv()

    def swap(layer, k, number, block, theirs=False):
        whose = 1 - core if theirs else core
        both = refs(layer, k, block, "all", whose=whose)
        return [
            pltpu.make_async_remote_copy(r, r, push.at[layer, k, number, i], pull.at[layer, k, number, i], device_id=partner, device_id_type=MESH)
            for i, r in enumerate(both)
        ]

    def to_partner(layer, k, number, block):
        for copy in swap(layer, k, number, block):
            copy.start()
            sent.append(copy)

    GROUPS = ((1, 0), (2, -1), (3, 1), (4, 2))

    def first(layer):
        for group in (0, 1):
            for k in (0, 1):
                for kind in (0, 1):
                    out(layer, k, group, kind, place(k, 0, 0), mine=True)

    def second(layer):
        for kind, off, group in ((0, -1, 2), (1, 1, 3)):
            for k in (0, 1):
                block = place(k, off, 0)
                arrived(layer, k, 0, kind, block)
                out(layer, k, 0, 2 + kind, block)
                out(layer, k, group, 0, block)
                out(layer, k, group, 1, block)
                to_partner(layer, k, kind, block)

    def passed(layer, group, i):
        for kind, off in ((0, -1), (1, 1)):
            for k in (0, 1):
                block = place(k, i, off)
                arrived(layer, k, group, kind, block)
                out(layer, k, group, 2 + kind, block)
                to_partner(layer, k, 3 * group + kind, block)

    def opposite(layer):
        for k in (0, 1):
            block = place(k, 2, 0)
            arrived(layer, k, 0, 2, block)
            arrived(layer, k, 0, 3, block)
            out(layer, k, 4, 0, block)
            out(layer, k, 4, 1, block)
            to_partner(layer, k, 2, block)

    def last(layer, group, i):
        for k in (0, 1):
            block = place(k, i, 2)
            arrived(layer, k, group, 2, block)
            arrived(layer, k, group, 3, block)
            to_partner(layer, k, 3 * group + 2, block)

    def pulled(layer):
        for k in (0, 1):
            for number, (i, j) in enumerate([(-1, 0), (1, 0), (2, 0)] + [(i, j) for _, i in GROUPS for j in (-1, 1, 2)]):
                for copy in swap(layer, k, number, place(k, i, j), theirs=True):
                    copy.wait_recv()

    first(0)
    for copy in owns:
        copy.start()
    for layer in range(layers):
        second(layer)
        passed(layer, 1, 0)
        opposite(layer)
        passed(layer, 2, -1)
        passed(layer, 3, 1)
        if layer + 1 < layers:
            first(layer + 1)
        passed(layer, 4, 2)
        for group, i in GROUPS:
            last(layer, group, i)
    for layer in range(layers):
        pulled(layer)
    for copy in owns:
        copy.wait()
    for copy in sent:
        copy.wait_send()


def gather(gu, d, n):
    layers = gu.shape[0]
    any_space = pl.BlockSpec(memory_space=pl.ANY)
    dma = pltpu.SemaphoreType.DMA
    return pl.pallas_call(
        functools.partial(gather_kernel, layers, n),
        out_shape=(
            jax.ShapeDtypeStruct((layers, 2, n, n) + gu.shape[2:], BF),
            jax.ShapeDtypeStruct((layers, d.shape[1], n, n) + d.shape[2:], BF),
        ),
        in_specs=[pl.BlockSpec(memory_space=pltpu.VMEM)] * 2,
        out_specs=(any_space, any_space),
        scratch_shapes=[dma((layers, 2, 5, 4, 2)), dma((layers, 2, 5, 4, 2)), dma((layers, 2, 15, 2)), dma((layers, 2, 15, 2)), dma((layers, 2))],
        compiler_params=pltpu.CompilerParams(collective_id=0, has_side_effects=True, vmem_limit_bytes=VMEM_LIMIT),
    )(gu, d)


def forward_kernel(h_ref, gate_ref, up_ref, down_ref, out_ref, a_ref, total_ref):
    number = pl.program_id(0)

    @pl.when(number == 0)
    def _():
        wide = h_ref[...].astype(F32)
        a_ref[...] = (wide * scale_of(wide)).astype(BF)
        total_ref[...] = jnp.zeros_like(total_ref)

    half = h_ref.shape[0] // 2
    for part in range(2):
        rows = pl.ds(part * half, half)
        gate = dot(a_ref[rows, :], gate_ref[0, 0])
        up = dot(a_ref[rows, :], up_ref[0, 0])
        act = (gate * jax.nn.sigmoid(gate) * up).astype(BF)
        total_ref[rows, :] += dot(act, down_ref[0])

    @pl.when(number == pl.num_programs(0) - 1)
    def _():
        out_ref[...] = (h_ref[...].astype(F32) + total_ref[...].astype(BF).astype(F32)).astype(BF)


def forward(h, gu, down, layer):
    tokens, d = h.shape
    ff = down.shape[1]
    whole = pl.BlockSpec((tokens, d), lambda j: (0, 0))
    return pl.pallas_call(
        forward_kernel,
        grid=(ff // TILE,),
        out_shape=jax.ShapeDtypeStruct((tokens, d), BF),
        in_specs=[
            whole,
            pl.BlockSpec((1, 1, d, TILE), lambda j: (layer, 0, 0, j)),
            pl.BlockSpec((1, 1, d, TILE), lambda j: (layer, 1, 0, j)),
            pl.BlockSpec((1, TILE, d), lambda j: (layer, j, 0)),
        ],
        out_specs=whole,
        scratch_shapes=[pltpu.VMEM((tokens, d), BF), pltpu.VMEM((tokens, d), F32)],
        compiler_params=pltpu.CompilerParams(vmem_limit_bytes=VMEM_LIMIT),
        cost_estimate=pl.CostEstimate(flops=6 * tokens * d * ff, bytes_accessed=6 * d * ff, transcendentals=tokens * ff),
    )(h, gu, gu, down)


def backward_kernel(layers, n, chunks, *refs):
    hs, (dy_ref, gu_ref, down_ref, grads_ref, squares_ref) = refs[:layers], refs[layers : layers + 5]
    a_ref, at_ref, by_ref, dag_ref, dau_ref, dg_ref, du_ref, act_ref = refs[layers + 5 : layers + 13]
    gub, downb, staged, relay1, side1, partial, relay2, side2, sq_ref, sq_all, send, recv, wsem, credit, sqs, sqr = refs[layers + 13 :]
    tokens, d = dy_ref.shape
    rounds = layers * chunks
    rows, lanes = staged.shape[-2], staged.shape[-1]
    quarter = lanes // 4
    torus = Torus(n)
    ways = [(a, b) for a in (0, 1) for b in (1, -1)]

    greet([torus.device(a, b) for a, b in ways] + [torus.device(a, 2) for a in (0, 1)])

    def source(slot, k, phase, dest, half):
        if phase == 1:
            return partial.at[slot, k, :, dest, :, pl.ds(half * quarter, quarter)]
        cols = pl.ds((2 * k + half) * quarter, quarter)
        return staged.at[slot, :, dest, :, :, cols] if k == 0 else staged.at[slot, :, :, dest, :, cols]

    def message(slot, k, phase, kind, way):
        axis = k if phase == 0 else 1 - k
        relay, side = (relay1, side1) if phase == 0 else (relay2, side2)
        half = 1 - way if kind == 1 else way
        to_side = side.at[slot, k, way, half]
        if kind == 0:
            src, dst = source(slot, k, phase, torus.step(axis, 2), half), relay.at[slot, k, way]
        elif kind == 1:
            src, dst = source(slot, k, phase, torus.step(axis, 1 - 2 * way), half), to_side
        else:
            src, dst = relay.at[slot, k, way], to_side
        at = (slot, k, phase, kind, way)
        return pltpu.make_async_remote_copy(src, dst, send.at[at], recv.at[at], device_id=torus.device(axis, 1 - 2 * way), device_id_type=MESH)

    def issue(slot, phase):
        for kind in (0, 1):
            for k in (0, 1):
                for way in (0, 1):
                    message(slot, k, phase, kind, way).start()

    def middle(slot, phase):
        for k in (0, 1):
            axis = k if phase == 0 else 1 - k
            for way in (0, 1):
                message(slot, k, phase, 0, way).wait_recv()
                mine = source(slot, k, phase, torus.step(axis, 1 - 2 * way), way)
                held = (relay1 if phase == 0 else relay2).at[slot, k, way]

                def add(i, _, mine=mine, held=held):
                    at = (i,) if phase == 1 else (lax.div(i, n), lax.rem(i, n))
                    held[at] = (held[at].astype(F32) + mine[at].astype(F32)).astype(BF)
                    return 0

                lax.fori_loop(0, 3 if phase == 1 else 3 * n, add, 0)
                message(slot, k, phase, 2, way).start()

    def finish(slot, phase, layer=None, chunk=None):
        for k in (0, 1):
            axis = k if phase == 0 else 1 - k
            for way in (0, 1):
                for kind in (1, 2):
                    message(slot, k, phase, kind, way).wait_recv()
            side = (side1 if phase == 0 else side2).at[slot, k]
            for half in (0, 1):
                mine = source(slot, k, phase, torus.step(axis, 0), half)
                cols = pl.ds(half * quarter, quarter)

                def add(i, _, mine=mine, half=half, cols=cols, k=k, side=side):
                    at = (i,) if phase == 1 else (lax.div(i, n), lax.rem(i, n))
                    total = mine[at].astype(F32) + side[(0, half) + at].astype(F32) + side[(1, half) + at].astype(F32)
                    total = total.astype(BF)
                    if phase == 0:
                        partial[(slot, k) + at + (slice(None), cols)] = total
                    else:
                        grads_ref[(layer, chunk) + at + (slice(None), pl.ds((2 * k + half) * quarter, quarter))] = total
                        sq_ref[...] += total.astype(F32) ** 2
                    return 0

                lax.fori_loop(0, 3 if phase == 1 else 3 * n, add, 0)
            for way in (0, 1):
                for kind in (0, 1, 2):
                    message(slot, k, phase, kind, way).wait_send()

    def give():
        for i, (a, b) in enumerate(ways):
            pl.semaphore_signal(credit.at[i ^ 1], inc=1, device_id=torus.device(a, b), device_id_type=MESH)

    def take():
        for i in range(4):
            pl.semaphore_wait(credit.at[i], 1)

    def fetch(layer, tile, slot):
        cols = pl.ds(pl.multiple_of(tile * TILE, TILE), TILE)
        return (
            pltpu.make_async_copy(gu_ref.at[layer, :, :, cols], gub.at[slot], wsem.at[slot, 0]),
            pltpu.make_async_copy(down_ref.at[layer, cols], downb.at[slot], wsem.at[slot, 1]),
        )

    def compute(layer, slot, t, buf):
        gate_w, up_w, down_w = gub[buf, 0], gub[buf, 1], downb[buf]
        half = tokens // 2
        for part in range(2):
            these = pl.ds(part * half, half)
            gate = dot(a_ref[these, :], gate_w)
            up = dot(a_ref[these, :], up_w)
            dact = dot(by_ref[these, :], down_w, (1, 1)).astype(BF).astype(F32)
            sig = jax.nn.sigmoid(gate)
            silu = gate * sig
            act_ref[these, :] = (silu * up).astype(BF)
            du_ref[these, :] = (dact * silu).astype(BF)
            dg_ref[these, :] = (dact * up * (sig * (1.0 + gate * (1.0 - sig)))).astype(BF)
        cols = pl.ds(pl.multiple_of(t * TILE, TILE), TILE)
        staged[slot, 0, :, :, :, cols] = dot(at_ref[...], dg_ref[...]).astype(BF).reshape(n, n, rows, TILE)
        staged[slot, 1, :, :, :, cols] = dot(at_ref[...], du_ref[...]).astype(BF).reshape(n, n, rows, TILE)
        by_down = dot(act_ref[...], by_ref[...], (0, 0)).astype(BF).reshape(n, lanes // d, rows, d)
        for m in range(lanes // d):
            staged[slot, 2, t, :, :, pl.ds(m * d, d)] = by_down[:, m]
        if layer > 0:
            dag_ref[...] += dot(dg_ref[...], gate_w, (1, 1))
            dau_ref[...] += dot(du_ref[...], up_w, (1, 1))

    per = lanes // TILE
    tiles = per * chunks
    sq_ref[...] = jnp.zeros_like(sq_ref)
    by_ref[...] = dy_ref[...]
    for copy in fetch(layers - 1, 0, 0):
        copy.start()

    for layer in reversed(range(layers)):
        before = (layers - 1 - layer) * chunks
        wide = hs[layer][...].astype(F32)
        normed = wide * scale_of(wide)
        a_ref[...] = normed.astype(BF)
        at_ref[...] = normed.T.astype(BF)
        if layer > 0:
            dag_ref[...] = jnp.zeros_like(dag_ref)
            dau_ref[...] = jnp.zeros_like(dau_ref)

        def tile_step(s, _, layer=layer, before=before):
            t, r = lax.rem(s, per), before + lax.div(s, per)
            buf, slot = lax.rem(s, 2), lax.rem(r, 2)
            other = 1 - slot

            for copy in fetch(layer, s, buf):
                copy.wait()

            @pl.when(s + 1 < tiles)
            def _():
                for copy in fetch(layer, s + 1, 1 - buf):
                    copy.start()

            compute(layer, slot, t, buf)

            @pl.when((t == 0) & (r >= 1))
            def _():
                middle(other, 0)

            @pl.when((t == 1) & (r >= 2))
            def _():
                middle(slot, 1)

            @pl.when((t == 2) & (r >= 2))
            def _():
                done = r - 2
                finish(slot, 1, layers - 1 - lax.div(done, chunks), lax.rem(done, chunks))
                give()

            @pl.when(t == per - 1)
            def _():
                @pl.when(r >= 2)
                def _():
                    take()

                issue(slot, 0)

                @pl.when(r >= 1)
                def _():
                    finish(other, 0)
                    issue(other, 1)

            return 0

        lax.fori_loop(0, tiles, tile_step, 0)
        if layer > 0:
            for copy in fetch(layer - 1, 0, 0):
                copy.start()

            def norm_back(i, _, layer=layer):
                these = pl.ds(pl.multiple_of(i * LANES, LANES), LANES)
                wide = hs[layer][these, :].astype(F32)
                scale = scale_of(wide)
                da = (dag_ref[these, :].astype(BF).astype(F32) + dau_ref[these, :].astype(BF).astype(F32)).astype(BF).astype(F32)
                along = jnp.mean(da * wide, -1, keepdims=True)
                back = (da * scale - wide * (scale * scale * scale * along)).astype(BF)
                by_ref[these, :] = (by_ref[these, :].astype(F32) + back.astype(F32)).astype(BF)
                return 0

            lax.fori_loop(0, tokens // LANES, norm_back, 0)

    end = rounds - 1
    middle(end % 2, 0)
    middle((end - 1) % 2, 1)
    finish((end - 1) % 2, 1, layers - 1 - (end - 1) // chunks, (end - 1) % chunks)
    finish(end % 2, 0)
    issue(end % 2, 1)
    middle(end % 2, 1)
    finish(end % 2, 1, layers - 1 - end // chunks, end % chunks)

    mine = jnp.sum(sq_ref[...], axis=0, keepdims=True)
    mine = sum(mine[:, i * LANES : (i + 1) * LANES] for i in range(quarter // LANES))
    sq_all[0, 0] = jnp.broadcast_to(mine, sq_all.shape[2:])
    for axis in (0, 1):
        copies = [
            pltpu.make_async_remote_copy(
                sq_all.at[axis, 0], sq_all.at[axis, 1 + i], sqs.at[axis, i], sqr.at[axis, i], device_id=torus.device(axis, by), device_id_type=MESH
            )
            for i, by in enumerate((1, 2, -1))
        ]
        for copy in copies:
            copy.start()
        for copy in copies:
            copy.wait()
        total = sum(sq_all[axis, i] for i in range(1, n)) + sq_all[axis, 0]
        if axis == 0:
            sq_all[1, 0] = total
        else:
            squares_ref[...] = total


def backward(hs, dy, gu, down, n, chunks):
    layers, (tokens, d), ff = len(hs), dy.shape, down.shape[1]
    lanes = ff // chunks
    rows = d // (n * n)
    quarter = lanes // 4
    vmem, anywhere = pl.BlockSpec(memory_space=pltpu.VMEM), pl.BlockSpec(memory_space=pl.ANY)
    dma = pltpu.SemaphoreType.DMA
    return pl.pallas_call(
        functools.partial(backward_kernel, layers, n, chunks),
        out_shape=(jax.ShapeDtypeStruct((layers, chunks, 3, rows, lanes), BF), jax.ShapeDtypeStruct((8, LANES), F32)),
        in_specs=[vmem] * (layers + 1) + [anywhere] * 2,
        out_specs=(vmem, vmem),
        scratch_shapes=[
            pltpu.VMEM((tokens, d), BF),
            pltpu.VMEM((d, tokens), BF),
            pltpu.VMEM((tokens, d), BF),
            pltpu.VMEM((tokens, d), F32),
            pltpu.VMEM((tokens, d), F32),
            pltpu.VMEM((tokens, TILE), BF),
            pltpu.VMEM((tokens, TILE), BF),
            pltpu.VMEM((tokens, TILE), BF),
            pltpu.VMEM((2, 2, d, TILE), BF),
            pltpu.VMEM((2, TILE, d), BF),
            pltpu.VMEM((2, 3, n, n, rows, lanes), BF),
            pltpu.VMEM((2, 2, 2, 3, n, rows, quarter), BF),
            pltpu.VMEM((2, 2, 2, 2, 3, n, rows, quarter), BF),
            pltpu.VMEM((2, 2, 3, n, rows, 2 * quarter), BF),
            pltpu.VMEM((2, 2, 2, 3, rows, quarter), BF),
            pltpu.VMEM((2, 2, 2, 2, 3, rows, quarter), BF),
            pltpu.VMEM((rows, quarter), F32),
            pltpu.VMEM((2, n, 8, LANES), F32),
            dma((2, 2, 2, 3, 2)),
            dma((2, 2, 2, 3, 2)),
            dma((2, 2)),
            pltpu.SemaphoreType.REGULAR((4,)),
            dma((2, n - 1)),
            dma((2, n - 1)),
        ],
        compiler_params=pltpu.CompilerParams(collective_id=1, has_side_effects=True, vmem_limit_bytes=VMEM_LIMIT),
        cost_estimate=pl.CostEstimate(flops=28 * tokens * d * ff, bytes_accessed=12 * d * ff, transcendentals=2 * tokens * ff),
    )(*hs, dy, gu, down)


def solution(mesh):
    group = mesh.shape["dp"]
    n = math.isqrt(group)
    assert n == 4 and n * n == group

    def step(x, dy, *arrays):
        weights, m, v = (arrays[i : i + 3] for i in (0, 3, 6))
        layers, rows, ff = weights[0].shape
        d = weights[2].shape[-1]
        tall = ff // group
        chunks = tall // LANES
        gu = jnp.stack([w.reshape(layers, rows, group, chunks, LANES).swapaxes(2, 3).reshape(layers, rows, ff) for w in weights[:2]], axis=1)
        gu, down = gather(gu.reshape(layers, 2, 2, rows // 2, ff), weights[2].reshape(layers, chunks, LANES, d), n)
        gu, down = gu.reshape(layers, 2, d, ff), down.reshape(layers, ff, d)
        h = x[0]
        kept = [h]
        for number in range(layers - 1):
            h = forward(h, gu, down, number)
            kept.append(h)
        grads, squares = backward(kept, dy[0], gu, down, n, chunks)
        gradients = [
            grads[:, :, i].reshape(layers, chunks, rows, group, LANES).transpose(0, 2, 3, 1, 4).reshape(layers, rows, ff).astype(F32) for i in range(2)
        ]
        last = grads[:, :, 2].reshape(layers, chunks, rows, ff // chunks // d, d).swapaxes(2, 3).reshape(layers, tall, d)
        gradients.append(last.astype(F32))
        gradients = clipped(gradients, jnp.sum(squares[0]), group * sum(g.size for g in gradients))
        new = [adamw(w.astype(F32), m, v, g) for w, m, v, g in zip(weights, m, v, gradients, strict=True)]
        return tuple(one[which] for which in range(3) for one in new)

    states, cut = P(("rep", "dp"), None, None), P(None, "dp", None)
    return jax.shard_map(
        step,
        mesh=mesh,
        in_specs=(states, states) + (cut,) * 9,
        out_specs=(P("rep", "dp", None),) * 9,
        check_vma=False,
    )
```

```python
import functools
import math

import jax
import jax.numpy as jnp
from jax import lax
from jax.experimental import pallas as pl
from jax.experimental.pallas import tpu as pltpu
from jax.sharding import PartitionSpec as P

MESH = pl.DeviceIdType.MESH
BF, F32 = jnp.bfloat16, jnp.float32
LANES = 128
TILE = 512
VMEM_LIMIT = 66_000_000
SIDES = (1, -1)


def dot(a, b, over=(1, 0)):
    return lax.dot_general(a, b, (((over[0],), (over[1],)), ((), ())), preferred_element_type=F32)


def scale_of(wide):
    return lax.rsqrt(jnp.mean(wide**2, -1, keepdims=True) + 1e-6)


def adamw(w, m, v, g):
    m = 0.9 * m + 0.1 * g
    v = 0.95 * v + 0.05 * g * g
    step = m * lax.rsqrt(v + 1e-8) + 0.1 * w
    return (w - 0.02 * step).astype(BF), m, v


class Torus:
    def __init__(self, n):
        me = lax.axis_index("dp")
        self.n = n
        self.at = (lax.div(me, n), lax.rem(me, n))

    def step(self, axis, by):
        return lax.rem(self.at[axis] + (by + self.n), self.n)

    def device(self, axis, by):
        x, y = self.at
        moved = self.step(axis, by)
        return {"dp": moved * self.n + y if axis == 0 else x * self.n + moved}


def greet(others):
    barrier = pltpu.get_barrier_semaphore()
    for other in others:
        pl.semaphore_signal(barrier, inc=1, device_id=other, device_id_type=MESH)
    pl.semaphore_wait(barrier, len(others))


def gather_kernel(layers, n, x_in, gu_in, d_in, gu_out, d_out, h_out, a_out, at_out, send, recv, push, pull, own, wsem, total_ref, gub, downb):
    torus = Torus(n)
    rep = lax.axis_index("rep")
    core = lax.rem(rep, 2)
    partner = {"rep": rep + 1 - 2 * core}
    lanes, rows = gu_in.shape[-1] // 2, d_in.shape[-2]
    tokens, d = x_in.shape
    parts = {"all": (0, 1), "a": (0, 2), "b": (1, 2)}

    def place(k, i, j):
        first, second = torus.step(k, i), torus.step(1 - k, j)
        return (first, second) if k == 0 else (second, first)

    def refs(layer, k, block, part, mine=False, whose=core):
        which, of = parts[part]
        wide, high = lanes // of, rows // of
        cols = pl.ds(k * lanes + which * wide, wide)
        tall = pl.ds(which * high, high)
        if mine:
            return gu_in.at[layer, :, whose, :, cols], d_in.at[layer, 2 * whose + k, tall]
        x, y = block
        return gu_out.at[layer, :, x, y, whose, :, cols], d_out.at[layer, 2 * whose + k, x, y, tall]

    greet([torus.device(a, b) for a in range(2) for b in SIDES] + [partner])

    def owns(layer):
        x, y = torus.at
        return (
            pltpu.make_async_copy(gu_in.at[layer], gu_out.at[layer, :, x, y], own.at[layer, 0]),
            pltpu.make_async_copy(d_in.at[layer], d_out.at[layer, :, x, y], own.at[layer, 1]),
        )

    sent = []

    def message(layer, k, group, kind, i, j):
        axis = k if group == 0 else 1 - k
        part = ("all", "all", "a", "b")[kind]
        target = torus.device(axis, SIDES[kind % 2])
        block = place(k, i, j)
        there = refs(layer, k, block, part)
        here = refs(layer, k, block, part, i == 0 and j == 0)
        return [
            pltpu.make_async_remote_copy(s, t, send.at[layer, k, group, kind, q], recv.at[layer, k, group, kind, q], device_id=target, device_id_type=MESH)
            for q, (s, t) in enumerate(zip(here, there, strict=True))
        ]

    def out(*which):
        for copy in message(*which):
            copy.start()
        sent.append((message, which))

    def arrived(*which):
        for copy in message(*which):
            copy.wait_recv()

    def swap(layer, k, number, i, j, theirs=False):
        whose = 1 - core if theirs else core
        both = refs(layer, k, place(k, i, j), "all", whose=whose)
        return [
            pltpu.make_async_remote_copy(r, r, push.at[layer, k, number, q], pull.at[layer, k, number, q], device_id=partner, device_id_type=MESH)
            for q, r in enumerate(both)
        ]

    def to_partner(*which):
        for copy in swap(*which):
            copy.start()
        sent.append((swap, which))

    GROUPS = ((1, 0), (2, -1), (3, 1), (4, 2))

    def first(layer):
        for group in range(2):
            for k in range(2):
                for kind in range(2):
                    out(layer, k, group, kind, 0, 0)

    def second(layer):
        for kind, off, group in ((0, -1, 2), (1, 1, 3)):
            for k in range(2):
                arrived(layer, k, 0, kind, off, 0)
                out(layer, k, 0, 2 + kind, off, 0)
                out(layer, k, group, 0, off, 0)
                out(layer, k, group, 1, off, 0)
                to_partner(layer, k, kind, off, 0)

    def passed(layer, group, i):
        for kind, off in ((0, -1), (1, 1)):
            for k in range(2):
                arrived(layer, k, group, kind, i, off)
                out(layer, k, group, 2 + kind, i, off)
                to_partner(layer, k, 3 * group + kind, i, off)

    def opposite(layer):
        for k in range(2):
            arrived(layer, k, 0, 2, 2, 0)
            arrived(layer, k, 0, 3, 2, 0)
            out(layer, k, 4, 0, 2, 0)
            out(layer, k, 4, 1, 2, 0)
            to_partner(layer, k, 2, 2, 0)

    def last(layer):
        for group, i in GROUPS:
            for k in range(2):
                arrived(layer, k, group, 2, i, 2)
                arrived(layer, k, group, 3, i, 2)
                to_partner(layer, k, 3 * group + 2, i, 2)

    def pulled(layer):
        for k in range(2):
            for number, (i, j) in enumerate([(-1, 0), (1, 0), (2, 0)] + [(i, j) for _, i in GROUPS for j in (-1, 1, 2)]):
                for copy in swap(layer, k, number, i, j, True):
                    copy.wait_recv()
        for copy in owns(layer):
            copy.wait()

    def stages(layer):
        def ahead():
            if layer + 1 < layers:
                first(layer + 1)
            passed(layer, 4, 2)

        return (
            lambda: second(layer),
            lambda: passed(layer, 1, 0),
            lambda: opposite(layer),
            lambda: passed(layer, 2, -1),
            lambda: passed(layer, 3, 1),
            ahead,
        )

    per = n
    tiles = d_out.shape[1] * per

    def fetch(layer, s, buf):
        cols = pl.ds(pl.multiple_of(s * TILE, TILE), TILE)
        return (
            pltpu.make_async_copy(gu_out.at[layer, :, :, :, :, :, cols], gub.at[buf], wsem.at[buf, 0]),
            pltpu.make_async_copy(d_out.at[layer, lax.div(s, per), lax.rem(s, per)], downb.at[buf], wsem.at[buf, 1]),
        )

    first(0)
    for layer in range(layers):
        for copy in owns(layer):
            copy.start()

    def enter(layer):
        wide = h_out[layer].astype(F32)
        wide = wide * scale_of(wide)
        a_out[layer] = wide.astype(BF)
        at_out[layer] = wide.T.astype(BF)

    h_out[0] = x_in[...]
    enter(0)
    for stage in stages(0):
        stage()
    last(0)
    pulled(0)

    for layer in range(layers - 1):
        todo = stages(layer + 1)
        total_ref[...] = jnp.zeros_like(total_ref)
        for copy in fetch(layer, 0, 0):
            copy.start()

        def tile_step(s, _, layer=layer, todo=todo):
            buf = lax.rem(s, 2)
            for copy in fetch(layer, s, buf):
                copy.wait()

            @pl.when(s + 1 < tiles)
            def _():
                for copy in fetch(layer, s + 1, 1 - buf):
                    copy.start()

            half = tokens // 2
            gate_w, up_w = gub[buf, 0].reshape(d, TILE), gub[buf, 1].reshape(d, TILE)
            for part in range(2):
                these = pl.ds(part * half, half)
                gate = dot(a_out[layer, these, :], gate_w)
                up = dot(a_out[layer, these, :], up_w)
                act = (gate * jax.nn.sigmoid(gate) * up).astype(BF)
                total_ref[these, :] += dot(act, downb[buf].reshape(TILE, d))

            for number, stage in enumerate(todo):
                pl.when(s == 2 * number + 1)(stage)
            return 0

        lax.fori_loop(0, tiles, tile_step, 0)
        h_out[layer + 1] = (h_out[layer].astype(F32) + total_ref[...].astype(BF).astype(F32)).astype(BF)
        enter(layer + 1)
        last(layer + 1)
        pulled(layer + 1)

    for make, which in sent:
        for copy in make(*which):
            copy.wait_send()


def gather(x, gu, d, n):
    layers, (tokens, wide) = gu.shape[0], x.shape
    anywhere, vmem = pl.BlockSpec(memory_space=pl.ANY), pl.BlockSpec(memory_space=pltpu.VMEM)
    dma = pltpu.SemaphoreType.DMA
    return pl.pallas_call(
        functools.partial(gather_kernel, layers, n),
        out_shape=(
            jax.ShapeDtypeStruct((layers, 2, n, n) + gu.shape[2:], BF),
            jax.ShapeDtypeStruct((layers, d.shape[1], n, n) + d.shape[2:], BF),
            jax.ShapeDtypeStruct((layers, tokens, wide), BF),
            jax.ShapeDtypeStruct((layers, tokens, wide), BF),
            jax.ShapeDtypeStruct((layers, wide, tokens), BF),
        ),
        in_specs=[vmem] * 3,
        out_specs=(anywhere, anywhere, vmem, vmem, vmem),
        scratch_shapes=[
            dma((layers, 2, 5, 4, 2)),
            dma((layers, 2, 5, 4, 2)),
            dma((layers, 2, 15, 2)),
            dma((layers, 2, 15, 2)),
            dma((layers, 2)),
            dma((2, 2)),
            pltpu.VMEM((tokens, wide), F32),
            pltpu.VMEM((2, 2, n, n) + gu.shape[2:-1] + (TILE,), BF),
            pltpu.VMEM((2, n) + d.shape[2:], BF),
        ],
        compiler_params=pltpu.CompilerParams(collective_id=0, has_side_effects=True, vmem_limit_bytes=VMEM_LIMIT),
    )(x, gu, d)


class Stream:
    def __init__(self, torus, slots, refs, result):
        self.torus, self.slots, self.result = torus, slots, result
        self.staged, relay1, side1, self.partial, relay2, side2, self.send, self.recv, self.credit = refs
        self.relay, self.side = (relay1, relay2), (side1, side2)
        self.quarter = self.staged.shape[-1] // 4

    def slot(self, r):
        return lax.rem(r, self.slots)

    def source(self, slot, k, phase, dest, half):
        q = self.quarter
        if phase == 1:
            return self.partial.at[slot, k, :, dest, :, pl.ds(half * q, q)]
        cols = pl.ds((2 * k + half) * q, q)
        return self.staged.at[slot, :, dest, :, :, cols] if k == 0 else self.staged.at[slot, :, :, dest, :, cols]

    def message(self, slot, k, phase, kind, way):
        torus = self.torus
        axis = k if phase == 0 else 1 - k
        half = 1 - way if kind == 1 else way
        held, to_side = self.relay[phase].at[slot, k, way], self.side[phase].at[slot, k, way, half]
        if kind == 0:
            src, dst = self.source(slot, k, phase, torus.step(axis, 2), half), held
        elif kind == 1:
            src, dst = self.source(slot, k, phase, torus.step(axis, SIDES[way]), half), to_side
        else:
            src, dst = held, to_side
        at = (slot, k, phase, kind, way)
        target = torus.device(axis, SIDES[way])
        return pltpu.make_async_remote_copy(src, dst, self.send.at[at], self.recv.at[at], device_id=target, device_id_type=MESH)

    def issue(self, r, phase):
        for kind in range(2):
            for k in range(2):
                for way in range(2):
                    self.message(self.slot(r), k, phase, kind, way).start()

    def middle(self, r, phase):
        slot = self.slot(r)
        for k in range(2):
            axis = k if phase == 0 else 1 - k
            for way in range(2):
                self.message(slot, k, phase, 0, way).wait_recv()
                mine = self.source(slot, k, phase, self.torus.step(axis, SIDES[way]), way)
                held = self.relay[phase].at[slot, k, way]
                held[...] = (held[...].astype(F32) + mine[...].astype(F32)).astype(BF)
                self.message(slot, k, phase, 2, way).start()

    def finish(self, r, phase):
        slot, q = self.slot(r), self.quarter
        for k in range(2):
            axis = k if phase == 0 else 1 - k
            for way in range(2):
                for kind in (1, 2):
                    self.message(slot, k, phase, kind, way).wait_recv()
            for half in range(2):
                mine = self.source(slot, k, phase, self.torus.step(axis, 0), half)
                side = self.side[phase]
                total = mine[...].astype(F32) + side[slot, k, 0, half].astype(F32) + side[slot, k, 1, half].astype(F32)
                if phase == 0:
                    self.partial[slot, k, :, :, :, pl.ds(half * q, q)] = total.astype(BF)
                else:
                    self.result(r, pl.ds((2 * k + half) * q, q), total.astype(BF))
            for way in range(2):
                for kind in (0, 1, 2):
                    self.message(slot, k, phase, kind, way).wait_send()

    def ways(self):
        return [(i, self.torus.device(a, b)) for i, (a, b) in enumerate((axis, side) for axis in range(2) for side in SIDES)]

    def give(self):
        for i, device in self.ways():
            pl.semaphore_signal(self.credit.at[i ^ 1], inc=1, device_id=device, device_id_type=MESH)

    def take(self):
        for i in range(4):
            pl.semaphore_wait(self.credit.at[i], 1)


LAG = 2
SLOTS = 5 * LAG


def backward_kernel(layers, n, *refs):
    hs_ref, a_ref, at_ref, dy_ref, gu_ref, down_ref, grads_ref, down_grads_ref, squares_ref, by_ref, dag_ref, dau_ref, dg_ref, du_ref, act_ref = refs[:15]
    gub, downb, wsem, sq_ref, sq_all, sqs, sqr, *stream = refs[15:]
    tokens, d = dy_ref.shape
    tiles, rows = grads_ref.shape[1], grads_ref.shape[3]
    per = n
    pairs = down_grads_ref.shape[2] // 2
    chunks, total_tiles = tiles // per, layers * tiles
    turns = per + pairs
    rounds = layers * chunks * turns
    torus = Torus(n)

    greet([torus.device(a, b) for a in range(2) for b in SIDES] + [torus.device(a, 2) for a in range(2)])

    def store(r, cols, total):
        chunk, turn = lax.div(r, turns), lax.rem(r, turns)
        layer, chunk = layers - 1 - lax.div(chunk, chunks), lax.rem(chunk, chunks)

        @pl.when(turn < per)
        def _():
            grads_ref[layer, chunk * per + turn, :, :, cols] = total

        @pl.when(turn >= per)
        def _():
            down_grads_ref[layer, chunk, pl.ds(2 * (turn - per), 2), :, cols] = total

        wide = total.astype(F32)
        sq_ref[...] += jnp.sum(wide * wide, axis=0)

    sums = Stream(torus, SLOTS, stream, store)

    def fetch(r, buf):
        layer, tile = layers - 1 - lax.div(r, tiles), lax.rem(r, tiles)
        cols = pl.ds(pl.multiple_of(tile * TILE, TILE), TILE)
        return (
            pltpu.make_async_copy(gu_ref.at[layer, :, :, cols], gub.at[buf], wsem.at[buf, 0]),
            pltpu.make_async_copy(down_ref.at[layer, cols], downb.at[buf], wsem.at[buf, 1]),
        )

    def norm_back(layer):
        def block(i, _):
            these = pl.ds(pl.multiple_of(i * LANES, LANES), LANES)
            wide = hs_ref[layer, these, :].astype(F32)
            scale = scale_of(wide)
            da = (dag_ref[these, :].astype(BF).astype(F32) + dau_ref[these, :].astype(BF).astype(F32)).astype(BF).astype(F32)
            along = jnp.mean(da * wide, -1, keepdims=True)
            back = (da * scale - wide * (scale * scale * scale * along)).astype(BF)
            by_ref[these, :] = (by_ref[these, :].astype(F32) + back.astype(F32)).astype(BF)
            return 0

        lax.fori_loop(0, tokens // LANES, block, 0)

    def compute(r, layer):
        buf, t = lax.rem(r, 2), lax.rem(r, per)
        first = lax.div(r, per) * turns
        gate_w, up_w, down_w = gub[buf, 0], gub[buf, 1], downb[buf]
        half = tokens // 2
        for part in range(2):
            these = pl.ds(part * half, half)
            gate = dot(a_ref[layer, these, :], gate_w)
            up = dot(a_ref[layer, these, :], up_w)
            dact = dot(by_ref[these, :], down_w, (1, 1)).astype(BF).astype(F32)
            sig = jax.nn.sigmoid(gate)
            silu = gate * sig
            act_ref[these, :] = (silu * up).astype(BF)
            du_ref[these, :] = (dact * silu).astype(BF)
            dg_ref[these, :] = (dact * up * (sig * (1.0 + gate * (1.0 - sig)))).astype(BF)
        for which, ref in enumerate((dg_ref, du_ref)):
            sums.staged[sums.slot(first + t), which] = dot(at_ref[layer], ref[...]).astype(BF).reshape(n, n, rows, TILE)
        by_down = dot(act_ref[...], by_ref[...], (0, 0)).astype(BF).reshape(n, 2 * pairs, rows, d)
        for m in range(2 * pairs):
            sums.staged[sums.slot(first + per + m // 2), m % 2, t] = by_down[:, m]

        @pl.when(layer > 0)
        def _():
            dag_ref[...] += dot(dg_ref[...], gate_w, (1, 1))
            dau_ref[...] += dot(du_ref[...], up_w, (1, 1))

    def turn(r, _):
        @pl.when(r < rounds)
        def _():
            @pl.when(r >= SLOTS)
            def _():
                sums.take()

            sums.issue(r, 0)

        def late(stages):
            return (r >= stages * LAG) & (r < rounds + stages * LAG)

        @pl.when(late(1))
        def _():
            sums.middle(r - LAG, 0)

        @pl.when(late(2))
        def _():
            sums.finish(r - 2 * LAG, 0)
            sums.issue(r - 2 * LAG, 1)

        @pl.when(late(3))
        def _():
            sums.middle(r - 3 * LAG, 1)

        @pl.when(late(4))
        def _():
            sums.finish(r - 4 * LAG, 1)

            @pl.when(r - 4 * LAG + SLOTS < rounds)
            def _():
                sums.give()

        return 0

    sq_ref[...] = jnp.zeros_like(sq_ref)
    by_ref[...] = dy_ref[...]
    for copy in fetch(0, 0):
        copy.start()

    def tile_step(r, _):
        t, first = lax.rem(r, per), lax.div(r, per) * turns

        @pl.when(r < total_tiles)
        def _():
            layer = layers - 1 - lax.div(r, tiles)
            for copy in fetch(r, lax.rem(r, 2)):
                copy.wait()

            @pl.when(r + 1 < total_tiles)
            def _():
                for copy in fetch(r + 1, 1 - lax.rem(r, 2)):
                    copy.start()

            @pl.when(lax.rem(r, tiles) == 0)
            def _():
                @pl.when(r > 0)
                def _():
                    norm_back(layer + 1)

                dag_ref[...] = jnp.zeros_like(dag_ref)
                dau_ref[...] = jnp.zeros_like(dau_ref)

            compute(r, layer)

        more = 1 + pairs * lax.div(t + 1, per) + (4 * LAG - 1) * lax.div(r, total_tiles)
        lax.fori_loop(first + t, first + t + more, turn, 0)
        return 0

    lax.fori_loop(0, total_tiles + 1, tile_step, 0)

    mine = jnp.sum(sq_ref[...], axis=0, keepdims=True)
    sq_all[0, 0] = jnp.broadcast_to(mine, sq_all.shape[2:])
    for axis in range(2):
        copies = [
            pltpu.make_async_remote_copy(
                sq_all.at[axis, 0], sq_all.at[axis, 1 + i], sqs.at[axis, i], sqr.at[axis, i], device_id=torus.device(axis, by), device_id_type=MESH
            )
            for i, by in enumerate((1, 2, -1))
        ]
        for copy in copies:
            copy.start()
        for copy in copies:
            copy.wait()
        total = sum(sq_all[axis, i] for i in range(1, n)) + sq_all[axis, 0]
        if axis == 0:
            sq_all[1, 0] = total
        else:
            squares_ref[...] = total


def backward(hs, normed, turned, dy, gu, down, n):
    layers, (tokens, d), ff = hs.shape[0], dy.shape, down.shape[1]
    rows, quarter, tiles = d // (n * n), TILE // 4, ff // TILE
    vmem, anywhere = pl.BlockSpec(memory_space=pltpu.VMEM), pl.BlockSpec(memory_space=pl.ANY)
    dma = pltpu.SemaphoreType.DMA

    both, block = (SLOTS, 2, 2), (2, n, rows, quarter)
    stream = [
        pltpu.VMEM((SLOTS, 2, n, n, rows, TILE), BF),
        pltpu.VMEM(both + block, BF),
        pltpu.VMEM(both + (2,) + block, BF),
        pltpu.VMEM((SLOTS, 2, 2, n, rows, 2 * quarter), BF),
        pltpu.VMEM(both + (2, rows, quarter), BF),
        pltpu.VMEM(both + (2, 2, rows, quarter), BF),
        dma(both + (3, 2)),
        dma(both + (3, 2)),
        pltpu.SemaphoreType.REGULAR((4,)),
    ]

    return pl.pallas_call(
        functools.partial(backward_kernel, layers, n),
        out_shape=(
            jax.ShapeDtypeStruct((layers, tiles, 2, rows, TILE), BF),
            jax.ShapeDtypeStruct((layers, tiles // n, LANES // rows, rows, d), BF),
            jax.ShapeDtypeStruct((8, LANES), F32),
        ),
        in_specs=[vmem] * 4 + [anywhere] * 2,
        out_specs=(vmem, vmem, vmem),
        scratch_shapes=[
            pltpu.VMEM((tokens, d), BF),
            pltpu.VMEM((tokens, d), F32),
            pltpu.VMEM((tokens, d), F32),
            pltpu.VMEM((tokens, TILE), BF),
            pltpu.VMEM((tokens, TILE), BF),
            pltpu.VMEM((tokens, TILE), BF),
            pltpu.VMEM((2, 2, d, TILE), BF),
            pltpu.VMEM((2, TILE, d), BF),
            dma((2, 2)),
            pltpu.VMEM((rows, quarter), F32),
            pltpu.VMEM((2, n, 8, LANES), F32),
            dma((2, n - 1)),
            dma((2, n - 1)),
        ]
        + stream,
        compiler_params=pltpu.CompilerParams(collective_id=1, has_side_effects=True, vmem_limit_bytes=VMEM_LIMIT),
        cost_estimate=pl.CostEstimate(flops=28 * tokens * d * ff, bytes_accessed=12 * d * ff, transcendentals=2 * tokens * ff),
    )(hs, normed, turned, dy, gu, down)


def update_kernel(count, n, grads_ref, down_grads_ref, squares_ref, *refs):
    w, m, v, new_w, new_m, new_v = (refs[i : i + 3] for i in range(0, 18, 3))
    squares = jnp.sum(squares_ref[0:1, :], axis=1, keepdims=True)
    factor = jnp.minimum(1.0, 0.5 * lax.rsqrt(squares / count + 1e-30))

    def put(which, at, g):
        new = adamw(w[which][at].astype(F32), m[which][at], v[which][at], g.astype(F32) * factor)
        for ref, value in zip((new_w[which], new_m[which], new_v[which]), new, strict=True):
            ref[at] = value

    t = pl.program_id(1)
    rows, span = w[0].shape[1:]
    for which in range(2):
        for y in range(n):
            for q in range(span // (n * LANES)):
                at = (0, slice(None), pl.ds((y * (span // (n * LANES)) + q) * LANES, LANES))
                put(which, at, grads_ref[0, q * n + t, which, :, pl.ds(y * LANES, LANES)])
    for i in range(down_grads_ref.shape[2]):
        put(2, (0, pl.ds(i * rows, rows)), down_grads_ref[0, 0, i])


def update(grads, down_grads, squares, weights, m, v, n, count):
    layers, rows, ff = weights[0].shape
    tall, d = weights[2].shape[1:]
    steps = n
    wide = pl.BlockSpec((1, rows, ff // steps), lambda l, t: (l, 0, t))
    high = pl.BlockSpec((1, tall // steps, d), lambda l, t: (l, t, 0))
    three = [wide, wide, high]
    shapes = [jax.ShapeDtypeStruct(w.shape, kind) for kind in (BF, F32, F32) for w in weights]
    return pl.pallas_call(
        functools.partial(update_kernel, count, n),
        grid=(layers, steps),
        out_shape=tuple(shapes),
        in_specs=[
            pl.BlockSpec((1,) + grads.shape[1:], lambda l, t: (l, 0, 0, 0, 0)),
            pl.BlockSpec((1, 1) + down_grads.shape[2:], lambda l, t: (l, t, 0, 0, 0)),
            pl.BlockSpec(squares.shape, lambda l, t: (0, 0)),
        ]
        + three * 3,
        out_specs=tuple(three * 3),
        compiler_params=pltpu.CompilerParams(vmem_limit_bytes=VMEM_LIMIT),
    )(grads, down_grads, squares, *weights, *m, *v)


def solution(mesh):
    group = mesh.shape["dp"]
    n = math.isqrt(group)
    assert n == 4 and n * n == group

    def step(x, dy, *arrays):
        weights, m, v = (arrays[i : i + 3] for i in (0, 3, 6))
        layers, rows, ff = weights[0].shape
        d = weights[2].shape[-1]
        tall = ff // group
        chunks = tall // LANES
        gu = jnp.stack([w.reshape(layers, rows, group, chunks, LANES).swapaxes(2, 3).reshape(layers, rows, ff) for w in weights[:2]], axis=1)
        gu, down, *states = gather(x[0], gu.reshape(layers, 2, 2, rows // 2, ff), weights[2].reshape(layers, chunks, LANES, d), n)
        gu, down = gu.reshape(layers, 2, d, ff), down.reshape(layers, ff, d)
        grads, down_grads, squares = backward(*states, dy[0], gu, down, n)
        return update(grads, down_grads, squares, weights, m, v, n, group * sum(w.size for w in weights))

    states, cut = P(("rep", "dp"), None, None), P(None, "dp", None)
    return jax.shard_map(
        step,
        mesh=mesh,
        in_specs=(states, states) + (cut,) * 9,
        out_specs=(P("rep", "dp", None),) * 9,
        check_vma=False,
    )
```

```python
import functools
import math

import jax
import jax.numpy as jnp
from jax import lax
from jax.experimental import pallas as pl
from jax.experimental.pallas import tpu as pltpu
from jax.sharding import PartitionSpec as P

MESH = pl.DeviceIdType.MESH
BF, F32 = jnp.bfloat16, jnp.float32
LANES = 128
TILE = 512
VMEM_LIMIT = 66_000_000
SIDES = (1, -1)


def dot(a, b, over=(1, 0)):
    return lax.dot_general(a, b, (((over[0],), (over[1],)), ((), ())), preferred_element_type=F32)


def scale_of(wide):
    return lax.rsqrt(jnp.mean(wide**2, -1, keepdims=True) + 1e-6)


def adamw(w, m, v, g):
    m = 0.9 * m + 0.1 * g
    v = 0.95 * v + 0.05 * g * g
    step = m * lax.rsqrt(v + 1e-8) + 0.1 * w
    return (w - 0.02 * step).astype(BF), m, v


class Torus:
    def __init__(self, n):
        me = lax.axis_index("dp")
        self.n = n
        self.at = (lax.div(me, n), lax.rem(me, n))

    def step(self, axis, by):
        return lax.rem(self.at[axis] + (by + self.n), self.n)

    def device(self, axis, by):
        x, y = self.at
        moved = self.step(axis, by)
        return {"dp": moved * self.n + y if axis == 0 else x * self.n + moved}


def greet(others):
    barrier = pltpu.get_barrier_semaphore()
    for other in others:
        pl.semaphore_signal(barrier, inc=1, device_id=other, device_id_type=MESH)
    pl.semaphore_wait(barrier, len(others))


def partner_core():
    rep = lax.axis_index("rep")
    return {"rep": rep + 1 - 2 * lax.rem(rep, 2)}


def gatherer(torus, units, gu_in, d_in, gu_out, d_out, send, recv, push, pull, own):
    core, partner = lax.rem(lax.axis_index("rep"), 2), partner_core()
    lanes, rows = gu_in.shape[-1] // d_in.shape[1], d_in.shape[2] // 2
    parts = {"all": (0, 1), "a": (0, 2), "b": (1, 2)}

    def place(k, i, j):
        first, second = torus.step(k, i), torus.step(1 - k, j)
        return (first, second) if k == 0 else (second, first)

    def refs(unit, k, block, part, mine=False, whose=core):
        layer, chunk = lax.div(unit, 2), lax.rem(unit, 2) * 2 + k
        which, of = parts[part]
        wide, high = lanes // of, rows // of
        cols = pl.ds(pl.multiple_of(chunk * lanes + which * wide, wide), wide)
        tall = pl.ds(pl.multiple_of(whose * rows + which * high, high), high)
        if mine:
            return gu_in.at[layer, :, whose, :, cols], d_in.at[layer, chunk, tall]
        x, y = block
        return gu_out.at[layer, :, x, y, whose, :, cols], d_out.at[layer, chunk, x, y, tall]

    def owns(layer):
        x, y = torus.at
        return (
            pltpu.make_async_copy(gu_in.at[layer], gu_out.at[layer, :, x, y], own.at[layer, 0]),
            pltpu.make_async_copy(d_in.at[layer], d_out.at[layer, :, x, y], own.at[layer, 1]),
        )

    sent = {}

    def message(unit, k, group, kind, i, j):
        axis = k if group == 0 else 1 - k
        part = ("all", "all", "a", "b")[kind]
        target = torus.device(axis, SIDES[kind % 2])
        block = place(k, i, j)
        there = refs(unit, k, block, part)
        here = refs(unit, k, block, part, i == 0 and j == 0)
        return [
            pltpu.make_async_remote_copy(s, t, send.at[unit, k, group, kind, q], recv.at[unit, k, group, kind, q], device_id=target, device_id_type=MESH)
            for q, (s, t) in enumerate(zip(here, there, strict=True))
        ]

    def out(*which):
        for copy in message(*which):
            copy.start()
        sent[message, which[1:]] = None

    def arrived(*which):
        for copy in message(*which):
            copy.wait_recv()

    def swap(unit, k, number, i, j, theirs=False):
        whose = 1 - core if theirs else core
        both = refs(unit, k, place(k, i, j), "all", whose=whose)
        return [
            pltpu.make_async_remote_copy(r, r, push.at[unit, k, number, q], pull.at[unit, k, number, q], device_id=partner, device_id_type=MESH)
            for q, r in enumerate(both)
        ]

    def to_partner(*which):
        for copy in swap(*which):
            copy.start()
        sent[swap, which[1:]] = None

    GROUPS = ((1, 0), (2, -1), (3, 1), (4, 2))

    def first(unit):
        for group in range(2):
            for k in range(2):
                for kind in range(2):
                    out(unit, k, group, kind, 0, 0)

    def second(unit):
        for kind, off, group in ((0, -1, 2), (1, 1, 3)):
            for k in range(2):
                arrived(unit, k, 0, kind, off, 0)
                out(unit, k, 0, 2 + kind, off, 0)
                out(unit, k, group, 0, off, 0)
                out(unit, k, group, 1, off, 0)
                to_partner(unit, k, kind, off, 0)

    def passed(unit, group, i):
        for kind, off in ((0, -1), (1, 1)):
            for k in range(2):
                arrived(unit, k, group, kind, i, off)
                out(unit, k, group, 2 + kind, i, off)
                to_partner(unit, k, 3 * group + kind, i, off)

    def opposite(unit):
        for k in range(2):
            arrived(unit, k, 0, 2, 2, 0)
            arrived(unit, k, 0, 3, 2, 0)
            out(unit, k, 4, 0, 2, 0)
            out(unit, k, 4, 1, 2, 0)
            to_partner(unit, k, 2, 2, 0)

    def last(unit):
        for group, i in GROUPS:
            for k in range(2):
                arrived(unit, k, group, 2, i, 2)
                arrived(unit, k, group, 3, i, 2)
                to_partner(unit, k, 3 * group + 2, i, 2)

    def pulled(unit):
        for k in range(2):
            for number, (i, j) in enumerate([(-1, 0), (1, 0), (2, 0)] + [(i, j) for _, i in GROUPS for j in (-1, 1, 2)]):
                for copy in swap(unit, k, number, i, j, True):
                    copy.wait_recv()

        @pl.when(lax.rem(unit, 2) == 0)
        def _():
            for copy in owns(lax.div(unit, 2)):
                copy.wait()

    def stages(unit):
        def ahead():
            pl.when(unit + 1 < units)(lambda: first(unit + 1))
            passed(unit, 4, 2)

        def end():
            last(unit)
            pulled(unit)

        return (
            lambda: second(unit),
            lambda: passed(unit, 1, 0),
            lambda: opposite(unit),
            lambda: passed(unit, 2, -1),
            lambda: passed(unit, 3, 1),
            ahead,
            end,
        )

    def start():
        first(0)
        for layer in range(units // 2):
            for copy in owns(layer):
                copy.start()

    def drain():
        def wait(unit, _):
            for make, which in sent:
                for copy in make(unit, *which):
                    copy.wait_send()
            return 0

        lax.fori_loop(0, units, wait, 0)

    return start, stages, drain


class Stream:
    def __init__(self, torus, slots, refs, result):
        self.torus, self.slots, self.result = torus, slots, result
        self.staged, relay1, side1, self.partial, relay2, side2, self.send, self.recv, self.credit = refs
        self.relay, self.side = (relay1, relay2), (side1, side2)
        self.quarter = self.staged.shape[-1] // 4

    def slot(self, r):
        return lax.rem(r, self.slots)

    def source(self, slot, k, phase, dest, half):
        q = self.quarter
        if phase == 1:
            return self.partial.at[slot, k, :, dest, :, pl.ds(half * q, q)]
        cols = pl.ds((2 * k + half) * q, q)
        return self.staged.at[slot, :, dest, :, :, cols] if k == 0 else self.staged.at[slot, :, :, dest, :, cols]

    def message(self, slot, k, phase, kind, way):
        torus = self.torus
        axis = k if phase == 0 else 1 - k
        half = 1 - way if kind == 1 else way
        held, to_side = self.relay[phase].at[slot, k, way], self.side[phase].at[slot, k, way, half]
        if kind == 0:
            src, dst = self.source(slot, k, phase, torus.step(axis, 2), half), held
        elif kind == 1:
            src, dst = self.source(slot, k, phase, torus.step(axis, SIDES[way]), half), to_side
        else:
            src, dst = held, to_side
        at = (slot, k, phase, kind, way)
        target = torus.device(axis, SIDES[way])
        return pltpu.make_async_remote_copy(src, dst, self.send.at[at], self.recv.at[at], device_id=target, device_id_type=MESH)

    def issue(self, r, phase):
        for kind in range(2):
            for k in range(2):
                for way in range(2):
                    self.message(self.slot(r), k, phase, kind, way).start()

    def middle(self, r, phase):
        slot = self.slot(r)
        for k in range(2):
            axis = k if phase == 0 else 1 - k
            for way in range(2):
                self.message(slot, k, phase, 0, way).wait_recv()
                mine = self.source(slot, k, phase, self.torus.step(axis, SIDES[way]), way)
                held = self.relay[phase].at[slot, k, way]
                held[...] = (held[...].astype(F32) + mine[...].astype(F32)).astype(BF)
                self.message(slot, k, phase, 2, way).start()

    def finish(self, r, phase):
        slot, q = self.slot(r), self.quarter
        for k in range(2):
            axis = k if phase == 0 else 1 - k
            for way in range(2):
                for kind in (1, 2):
                    self.message(slot, k, phase, kind, way).wait_recv()
            for half in range(2):
                mine = self.source(slot, k, phase, self.torus.step(axis, 0), half)
                side = self.side[phase]
                total = mine[...].astype(F32) + side[slot, k, 0, half].astype(F32) + side[slot, k, 1, half].astype(F32)
                if phase == 0:
                    self.partial[slot, k, :, :, :, pl.ds(half * q, q)] = total.astype(BF)
                else:
                    self.result(r, pl.ds((2 * k + half) * q, q), total.astype(BF))
            for way in range(2):
                for kind in (0, 1, 2):
                    self.message(slot, k, phase, kind, way).wait_send()

    def ways(self):
        return [(i, self.torus.device(a, b)) for i, (a, b) in enumerate((axis, side) for axis in range(2) for side in SIDES)]

    def give(self):
        for i, device in self.ways():
            pl.semaphore_signal(self.credit.at[i ^ 1], inc=1, device_id=device, device_id_type=MESH)

    def take(self):
        for i in range(4):
            pl.semaphore_wait(self.credit.at[i], 1)


LAG = 2
SLOTS = 5 * LAG


def step_kernel(layers, n, *refs):
    x_ref, dy_ref, gu_in, d_in, gu_ref, down_ref, grads_ref, down_grads_ref, squares_ref = refs[:9]
    hs_ref, a_ref, at_ref, by_ref, dag_ref, dau_ref, dg_ref, du_ref, act_ref, gub, downb, wsem, sq_ref, sq_all, sqs, sqr = refs[9:25]
    tokens, d = dy_ref.shape
    tiles, rows = grads_ref.shape[1], grads_ref.shape[3]
    per = n
    pairs = down_grads_ref.shape[2] // 2
    chunks, total_tiles = tiles // per, layers * tiles
    turns = per + pairs
    rounds = layers * chunks * turns
    torus = Torus(n)

    greet([torus.device(a, b) for a in range(2) for b in SIDES] + [torus.device(a, 2) for a in range(2)] + [partner_core()])

    start, stages, drain = gatherer(torus, 2 * layers, gu_in, d_in, gu_ref, down_ref, *refs[25:30])

    def enter(layer):
        wide = hs_ref[layer].astype(F32)
        wide = wide * scale_of(wide)
        a_ref[layer] = wide.astype(BF)
        at_ref[layer] = wide.T.astype(BF)

    def store(r, cols, total):
        chunk, turn = lax.div(r, turns), lax.rem(r, turns)
        layer, chunk = layers - 1 - lax.div(chunk, chunks), lax.rem(chunk, chunks)

        @pl.when(turn < per)
        def _():
            grads_ref[layer, chunk * per + turn, :, :, cols] = total

        @pl.when(turn >= per)
        def _():
            down_grads_ref[layer, chunk, pl.ds(2 * (turn - per), 2), :, cols] = total

        wide = total.astype(F32)
        sq_ref[...] += jnp.sum(wide * wide, axis=0)

    sums = Stream(torus, SLOTS, refs[30:], store)

    def fetch(layer, tile, buf):
        cols = pl.ds(pl.multiple_of(tile * TILE, TILE), TILE)
        return (
            pltpu.make_async_copy(gu_ref.at[layer, :, :, :, :, :, cols], gub.at[buf], wsem.at[buf, 0]),
            pltpu.make_async_copy(down_ref.at[layer, lax.div(tile, per), lax.rem(tile, per)], downb.at[buf], wsem.at[buf, 1]),
        )

    def begin(copies):
        for copy in copies:
            copy.start()

    def weights(buf):
        return gub[buf, 0].reshape(d, TILE), gub[buf, 1].reshape(d, TILE), downb[buf].reshape(TILE, d)

    def forward(layer):
        half, span = tokens // 2, tiles // 2
        dag_ref[...] = jnp.zeros_like(dag_ref)
        if layer > 0:
            begin(fetch(layer, 0, 0))

        def tile_step(i, _):
            s = i - span
            buf = lax.rem(i, 2)

            @pl.when(s >= 0)
            def _():
                for copy in fetch(layer, s, buf):
                    copy.wait()

            @pl.when((s + 1 >= 0) & (s + 1 < tiles))
            def _():
                begin(fetch(layer, s + 1, 1 - buf))

            @pl.when(s >= 0)
            def _():
                gate_w, up_w, down_w = weights(buf)
                for part in range(2):
                    these = pl.ds(part * half, half)
                    gate = dot(a_ref[layer, these, :], gate_w)
                    up = dot(a_ref[layer, these, :], up_w)
                    act = (gate * jax.nn.sigmoid(gate) * up).astype(BF)
                    dag_ref[these, :] += dot(act, down_w)

            for number, stage in enumerate(stages(2 * layer + lax.div(i, span))):
                pl.when(lax.rem(i, span) == number)(stage)
            return 0

        lax.fori_loop(span if layer > 0 else 0, span + tiles, tile_step, 0)
        hs_ref[layer + 1] = (hs_ref[layer].astype(F32) + dag_ref[...].astype(BF).astype(F32)).astype(BF)
        enter(layer + 1)

    def norm_back(layer):
        def block(i, _):
            these = pl.ds(pl.multiple_of(i * LANES, LANES), LANES)
            wide = hs_ref[layer, these, :].astype(F32)
            scale = scale_of(wide)
            da = (dag_ref[these, :].astype(BF).astype(F32) + dau_ref[these, :].astype(BF).astype(F32)).astype(BF).astype(F32)
            along = jnp.mean(da * wide, -1, keepdims=True)
            back = (da * scale - wide * (scale * scale * scale * along)).astype(BF)
            by_ref[these, :] = (by_ref[these, :].astype(F32) + back.astype(F32)).astype(BF)
            return 0

        lax.fori_loop(0, tokens // LANES, block, 0)

    def compute(r, layer):
        buf, t = lax.rem(r, 2), lax.rem(r, per)
        first = lax.div(r, per) * turns
        gate_w, up_w, down_w = weights(buf)
        half = tokens // 2
        for part in range(2):
            these = pl.ds(part * half, half)
            gate = dot(a_ref[layer, these, :], gate_w)
            up = dot(a_ref[layer, these, :], up_w)
            dact = dot(by_ref[these, :], down_w, (1, 1)).astype(BF).astype(F32)
            sig = jax.nn.sigmoid(gate)
            silu = gate * sig
            act_ref[these, :] = (silu * up).astype(BF)
            du_ref[these, :] = (dact * silu).astype(BF)
            dg_ref[these, :] = (dact * up * (sig * (1.0 + gate * (1.0 - sig)))).astype(BF)
        for which, ref in enumerate((dg_ref, du_ref)):
            sums.staged[sums.slot(first + t), which] = dot(at_ref[layer], ref[...]).astype(BF).reshape(n, n, rows, TILE)
        by_down = dot(act_ref[...], by_ref[...], (0, 0)).astype(BF).reshape(n, 2 * pairs, rows, d)
        for m in range(2 * pairs):
            sums.staged[sums.slot(first + per + m // 2), m % 2, t] = by_down[:, m]

        @pl.when(layer > 0)
        def _():
            dag_ref[...] += dot(dg_ref[...], gate_w, (1, 1))
            dau_ref[...] += dot(du_ref[...], up_w, (1, 1))

    def turn(r, _):
        @pl.when(r < rounds)
        def _():
            @pl.when(r >= SLOTS)
            def _():
                sums.take()

            sums.issue(r, 0)

        def late(stages):
            return (r >= stages * LAG) & (r < rounds + stages * LAG)

        @pl.when(late(1))
        def _():
            sums.middle(r - LAG, 0)

        @pl.when(late(2))
        def _():
            sums.finish(r - 2 * LAG, 0)
            sums.issue(r - 2 * LAG, 1)

        @pl.when(late(3))
        def _():
            sums.middle(r - 3 * LAG, 1)

        @pl.when(late(4))
        def _():
            sums.finish(r - 4 * LAG, 1)

            @pl.when(r - 4 * LAG + SLOTS < rounds)
            def _():
                sums.give()

        return 0

    sq_ref[...] = jnp.zeros_like(sq_ref)
    by_ref[...] = dy_ref[...]
    start()
    hs_ref[0] = x_ref[...]
    enter(0)
    for layer in range(layers - 1):
        forward(layer)
    begin(fetch(layers - 1, 0, 0))

    def tile_step(r, _):
        t, first = lax.rem(r, per), lax.div(r, per) * turns

        @pl.when(r < total_tiles)
        def _():
            layer = layers - 1 - lax.div(r, tiles)
            for copy in fetch(layer, lax.rem(r, tiles), lax.rem(r, 2)):
                copy.wait()

            @pl.when(r + 1 < total_tiles)
            def _():
                begin(fetch(layers - 1 - lax.div(r + 1, tiles), lax.rem(r + 1, tiles), 1 - lax.rem(r, 2)))

            @pl.when(lax.rem(r, tiles) == 0)
            def _():
                @pl.when(r > 0)
                def _():
                    norm_back(layer + 1)

                dag_ref[...] = jnp.zeros_like(dag_ref)
                dau_ref[...] = jnp.zeros_like(dau_ref)

            compute(r, layer)

        for number, stage in enumerate(stages(2 * layers - 1)):
            pl.when(r == number)(stage)

        more = 1 + pairs * lax.div(t + 1, per) + (4 * LAG - 1) * lax.div(r, total_tiles)
        lax.fori_loop(first + t, first + t + more, turn, 0)
        return 0

    lax.fori_loop(0, total_tiles + 1, tile_step, 0)
    drain()

    mine = jnp.sum(sq_ref[...], axis=0, keepdims=True)
    sq_all[0, 0] = jnp.broadcast_to(mine, sq_all.shape[2:])
    for axis in range(2):
        copies = [
            pltpu.make_async_remote_copy(
                sq_all.at[axis, 0], sq_all.at[axis, 1 + i], sqs.at[axis, i], sqr.at[axis, i], device_id=torus.device(axis, by), device_id_type=MESH
            )
            for i, by in enumerate((1, 2, -1))
        ]
        for copy in copies:
            copy.start()
        for copy in copies:
            copy.wait()
        total = sum(sq_all[axis, i] for i in range(1, n)) + sq_all[axis, 0]
        if axis == 0:
            sq_all[1, 0] = total
        else:
            squares_ref[...] = total


def gradients(x, dy, gu, down, n):
    layers, chunks, (tokens, d), ff = gu.shape[0], down.shape[1], x.shape, gu.shape[-1]
    rows, quarter, tiles = d // (n * n), TILE // 4, ff // TILE
    vmem, anywhere = pl.BlockSpec(memory_space=pltpu.VMEM), pl.BlockSpec(memory_space=pl.ANY)
    dma = pltpu.SemaphoreType.DMA

    both, block = (SLOTS, 2, 2), (2, n, rows, quarter)
    stream = [
        pltpu.VMEM((SLOTS, 2, n, n, rows, TILE), BF),
        pltpu.VMEM(both + block, BF),
        pltpu.VMEM(both + (2,) + block, BF),
        pltpu.VMEM((SLOTS, 2, 2, n, rows, 2 * quarter), BF),
        pltpu.VMEM(both + (2, rows, quarter), BF),
        pltpu.VMEM(both + (2, 2, rows, quarter), BF),
        dma(both + (3, 2)),
        dma(both + (3, 2)),
        pltpu.SemaphoreType.REGULAR((4,)),
    ]

    return pl.pallas_call(
        functools.partial(step_kernel, layers, n),
        out_shape=(
            jax.ShapeDtypeStruct((layers, 2, n, n) + gu.shape[2:], BF),
            jax.ShapeDtypeStruct((layers, chunks, n, n) + down.shape[2:], BF),
            jax.ShapeDtypeStruct((layers, tiles, 2, rows, TILE), BF),
            jax.ShapeDtypeStruct((layers, chunks, LANES // rows, rows, d), BF),
            jax.ShapeDtypeStruct((8, LANES), F32),
        ),
        in_specs=[vmem] * 4,
        out_specs=(anywhere, anywhere, vmem, vmem, vmem),
        scratch_shapes=[
            pltpu.VMEM((layers, tokens, d), BF),
            pltpu.VMEM((layers, tokens, d), BF),
            pltpu.VMEM((layers, d, tokens), BF),
            pltpu.VMEM((tokens, d), BF),
            pltpu.VMEM((tokens, d), F32),
            pltpu.VMEM((tokens, d), F32),
            pltpu.VMEM((tokens, TILE), BF),
            pltpu.VMEM((tokens, TILE), BF),
            pltpu.VMEM((tokens, TILE), BF),
            pltpu.VMEM((2, 2, n, n) + gu.shape[2:-1] + (TILE,), BF),
            pltpu.VMEM((2, n) + down.shape[2:], BF),
            dma((2, 2)),
            pltpu.VMEM((rows, quarter), F32),
            pltpu.VMEM((2, n, 8, LANES), F32),
            dma((2, n - 1)),
            dma((2, n - 1)),
            dma((2 * layers, 2, 5, 4, 2)),
            dma((2 * layers, 2, 5, 4, 2)),
            dma((2 * layers, 2, 15, 2)),
            dma((2 * layers, 2, 15, 2)),
            dma((layers, 2)),
        ]
        + stream,
        compiler_params=pltpu.CompilerParams(collective_id=0, has_side_effects=True, vmem_limit_bytes=VMEM_LIMIT),
        cost_estimate=pl.CostEstimate(flops=34 * tokens * d * ff, bytes_accessed=18 * d * ff, transcendentals=3 * tokens * ff),
    )(x, dy, gu, down)


def update_kernel(count, n, grads_ref, down_grads_ref, squares_ref, *refs):
    w, m, v, new_w, new_m, new_v = (refs[i : i + 3] for i in range(0, 18, 3))
    squares = jnp.sum(squares_ref[0:1, :], axis=1, keepdims=True)
    factor = jnp.minimum(1.0, 0.5 * lax.rsqrt(squares / count + 1e-30))

    def put(which, at, g):
        new = adamw(w[which][at].astype(F32), m[which][at], v[which][at], g.astype(F32) * factor)
        for ref, value in zip((new_w[which], new_m[which], new_v[which]), new, strict=True):
            ref[at] = value

    t = pl.program_id(1)
    rows, span = w[0].shape[1:]
    for which in range(2):
        for y in range(n):
            for q in range(span // (n * LANES)):
                at = (0, slice(None), pl.ds((y * (span // (n * LANES)) + q) * LANES, LANES))
                put(which, at, grads_ref[0, q * n + t, which, :, pl.ds(y * LANES, LANES)])
    for i in range(down_grads_ref.shape[2]):
        put(2, (0, pl.ds(i * rows, rows)), down_grads_ref[0, 0, i])


def update(grads, down_grads, squares, weights, m, v, n, count):
    layers, rows, ff = weights[0].shape
    tall, d = weights[2].shape[1:]
    steps = n
    wide = pl.BlockSpec((1, rows, ff // steps), lambda l, t: (l, 0, t))
    high = pl.BlockSpec((1, tall // steps, d), lambda l, t: (l, t, 0))
    three = [wide, wide, high]
    shapes = [jax.ShapeDtypeStruct(w.shape, kind) for kind in (BF, F32, F32) for w in weights]
    return pl.pallas_call(
        functools.partial(update_kernel, count, n),
        grid=(layers, steps),
        out_shape=tuple(shapes),
        in_specs=[
            pl.BlockSpec((1,) + grads.shape[1:], lambda l, t: (l, 0, 0, 0, 0)),
            pl.BlockSpec((1, 1) + down_grads.shape[2:], lambda l, t: (l, t, 0, 0, 0)),
            pl.BlockSpec(squares.shape, lambda l, t: (0, 0)),
        ]
        + three * 3,
        out_specs=tuple(three * 3),
        compiler_params=pltpu.CompilerParams(vmem_limit_bytes=VMEM_LIMIT),
    )(grads, down_grads, squares, *weights, *m, *v)


def solution(mesh):
    group = mesh.shape["dp"]
    n = math.isqrt(group)
    assert n == 4 and n * n == group

    def step(x, dy, *arrays):
        weights, m, v = (arrays[i : i + 3] for i in (0, 3, 6))
        layers, rows, ff = weights[0].shape
        d = weights[2].shape[-1]
        tall = ff // group
        chunks = tall // LANES
        gu = jnp.stack([w.reshape(layers, rows, group, chunks, LANES).swapaxes(2, 3).reshape(layers, rows, ff) for w in weights[:2]], axis=1)
        gu, down = gu.reshape(layers, 2, 2, rows // 2, ff), weights[2].reshape(layers, chunks, LANES, d)
        _, _, grads, down_grads, squares = gradients(x[0], dy[0], gu, down, n)
        return update(grads, down_grads, squares, weights, m, v, n, group * sum(w.size for w in weights))

    states, cut = P(("rep", "dp"), None, None), P(None, "dp", None)
    return jax.shard_map(
        step,
        mesh=mesh,
        in_specs=(states, states) + (cut,) * 9,
        out_specs=(P("rep", "dp", None),) * 9,
        check_vma=False,
    )
```

```python
import functools
import math

import jax
import jax.numpy as jnp
from jax import lax
from jax.experimental import pallas as pl
from jax.experimental.pallas import tpu as pltpu
from jax.sharding import PartitionSpec as P

MESH = pl.DeviceIdType.MESH
BF, F32 = jnp.bfloat16, jnp.float32
LANES = 128
TILE = 512
VMEM_LIMIT = 66_000_000
SIDES = (1, -1)


def dot(a, b, over=(1, 0)):
    return lax.dot_general(a, b, (((over[0],), (over[1],)), ((), ())), preferred_element_type=F32)


def scale_of(wide):
    return lax.rsqrt(jnp.mean(wide**2, -1, keepdims=True) + 1e-6)


def adamw(w, m, v, g):
    m = 0.9 * m + 0.1 * g
    v = 0.95 * v + 0.05 * g * g
    step = m * lax.rsqrt(v + 1e-8) + 0.1 * w
    return (w - 0.02 * step).astype(BF), m, v


class Torus:
    def __init__(self, n):
        me = lax.axis_index("dp")
        self.n = n
        self.at = (lax.div(me, n), lax.rem(me, n))

    def step(self, axis, by):
        return lax.rem(self.at[axis] + (by + self.n), self.n)

    def device(self, axis, by):
        x, y = self.at
        moved = self.step(axis, by)
        return {"dp": moved * self.n + y if axis == 0 else x * self.n + moved}


def greet(others):
    barrier = pltpu.get_barrier_semaphore()
    for other in others:
        pl.semaphore_signal(barrier, inc=1, device_id=other, device_id_type=MESH)
    pl.semaphore_wait(barrier, len(others))


def partner_core():
    rep = lax.axis_index("rep")
    return {"rep": rep + 1 - 2 * lax.rem(rep, 2)}


def gatherer(torus, units, gu_in, d_in, gu_out, d_out, send, recv, push, pull, own):
    core, partner = lax.rem(lax.axis_index("rep"), 2), partner_core()
    lanes, rows = gu_in.shape[-1] // d_in.shape[1], d_in.shape[2] // 2
    parts = {"all": (0, 1), "a": (0, 2), "b": (1, 2)}

    def place(k, i, j):
        first, second = torus.step(k, i), torus.step(1 - k, j)
        return (first, second) if k == 0 else (second, first)

    def refs(unit, k, block, part, mine=False, whose=core):
        layer, chunk = lax.div(unit, 2), lax.rem(unit, 2) * 2 + k
        which, of = parts[part]
        wide, high = lanes // of, rows // of
        cols = pl.ds(pl.multiple_of(chunk * lanes + which * wide, wide), wide)
        tall = pl.ds(pl.multiple_of(whose * rows + which * high, high), high)
        if mine:
            return gu_in.at[layer, :, whose, :, cols], d_in.at[layer, chunk, tall]
        x, y = block
        return gu_out.at[layer, :, x, y, whose, :, cols], d_out.at[layer, chunk, x, y, tall]

    def owns(layer):
        x, y = torus.at
        return (
            pltpu.make_async_copy(gu_in.at[layer], gu_out.at[layer, :, x, y], own.at[layer, 0]),
            pltpu.make_async_copy(d_in.at[layer], d_out.at[layer, :, x, y], own.at[layer, 1]),
        )

    sent = {}

    def message(unit, k, group, kind, i, j):
        axis = k if group == 0 else 1 - k
        part = ("all", "all", "a", "b")[kind]
        target = torus.device(axis, SIDES[kind % 2])
        block = place(k, i, j)
        there = refs(unit, k, block, part)
        here = refs(unit, k, block, part, i == 0 and j == 0)
        return [
            pltpu.make_async_remote_copy(s, t, send.at[unit, k, group, kind, q], recv.at[unit, k, group, kind, q], device_id=target, device_id_type=MESH)
            for q, (s, t) in enumerate(zip(here, there, strict=True))
        ]

    def out(*which):
        for copy in message(*which):
            copy.start()
        sent[message, which[1:]] = None

    def arrived(*which):
        for copy in message(*which):
            copy.wait_recv()

    def swap(unit, k, number, i, j, theirs=False):
        whose = 1 - core if theirs else core
        both = refs(unit, k, place(k, i, j), "all", whose=whose)
        return [
            pltpu.make_async_remote_copy(r, r, push.at[unit, k, number, q], pull.at[unit, k, number, q], device_id=partner, device_id_type=MESH)
            for q, r in enumerate(both)
        ]

    def to_partner(*which):
        for copy in swap(*which):
            copy.start()
        sent[swap, which[1:]] = None

    GROUPS = ((1, 0), (2, -1), (3, 1), (4, 2))

    def first(unit):
        for group in range(2):
            for k in range(2):
                for kind in range(2):
                    out(unit, k, group, kind, 0, 0)

    def second(unit):
        for kind, off, group in ((0, -1, 2), (1, 1, 3)):
            for k in range(2):
                arrived(unit, k, 0, kind, off, 0)
                out(unit, k, 0, 2 + kind, off, 0)
                out(unit, k, group, 0, off, 0)
                out(unit, k, group, 1, off, 0)
                to_partner(unit, k, kind, off, 0)

    def passed(unit, group, i):
        for kind, off in ((0, -1), (1, 1)):
            for k in range(2):
                arrived(unit, k, group, kind, i, off)
                out(unit, k, group, 2 + kind, i, off)
                to_partner(unit, k, 3 * group + kind, i, off)

    def opposite(unit):
        for k in range(2):
            arrived(unit, k, 0, 2, 2, 0)
            arrived(unit, k, 0, 3, 2, 0)
            out(unit, k, 4, 0, 2, 0)
            out(unit, k, 4, 1, 2, 0)
            to_partner(unit, k, 2, 2, 0)

    def last(unit):
        for group, i in GROUPS:
            for k in range(2):
                arrived(unit, k, group, 2, i, 2)
                arrived(unit, k, group, 3, i, 2)
                to_partner(unit, k, 3 * group + 2, i, 2)

    def pulled(unit):
        for k in range(2):
            for number, (i, j) in enumerate([(-1, 0), (1, 0), (2, 0)] + [(i, j) for _, i in GROUPS for j in (-1, 1, 2)]):
                for copy in swap(unit, k, number, i, j, True):
                    copy.wait_recv()

        @pl.when(lax.rem(unit, 2) == 0)
        def _():
            for copy in owns(lax.div(unit, 2)):
                copy.wait()

    def stages(unit):
        def ahead():
            pl.when(unit + 1 < units)(lambda: first(unit + 1))
            passed(unit, 4, 2)

        def end():
            last(unit)
            pulled(unit)

        return (
            lambda: second(unit),
            lambda: passed(unit, 1, 0),
            lambda: opposite(unit),
            lambda: passed(unit, 2, -1),
            lambda: passed(unit, 3, 1),
            ahead,
            end,
        )

    def start():
        first(0)
        for layer in range(units // 2):
            for copy in owns(layer):
                copy.start()

    def drain():
        def wait(unit, _):
            for make, which in sent:
                for copy in make(unit, *which):
                    copy.wait_send()
            return 0

        lax.fori_loop(0, units, wait, 0)

    return start, stages, drain


class Stream:
    def __init__(self, torus, slots, refs, result):
        self.torus, self.slots, self.result = torus, slots, result
        self.staged, relay1, side1, self.partial, relay2, side2, self.send, self.recv, self.credit = refs
        self.relay, self.side = (relay1, relay2), (side1, side2)
        self.quarter = self.staged.shape[-1] // 4

    def slot(self, r):
        return lax.rem(r, self.slots)

    def source(self, slot, k, phase, dest, half):
        q = self.quarter
        if phase == 1:
            return self.partial.at[slot, k, :, dest, :, pl.ds(half * q, q)]
        cols = pl.ds((2 * k + half) * q, q)
        return self.staged.at[slot, :, dest, :, :, cols] if k == 0 else self.staged.at[slot, :, :, dest, :, cols]

    def message(self, slot, k, phase, kind, way):
        torus = self.torus
        axis = k if phase == 0 else 1 - k
        half = 1 - way if kind == 1 else way
        held, to_side = self.relay[phase].at[slot, k, way], self.side[phase].at[slot, k, way, half]
        if kind == 0:
            src, dst = self.source(slot, k, phase, torus.step(axis, 2), half), held
        elif kind == 1:
            src, dst = self.source(slot, k, phase, torus.step(axis, SIDES[way]), half), to_side
        else:
            src, dst = held, to_side
        at = (slot, k, phase, kind, way)
        target = torus.device(axis, SIDES[way])
        return pltpu.make_async_remote_copy(src, dst, self.send.at[at], self.recv.at[at], device_id=target, device_id_type=MESH)

    def issue(self, r, phase):
        for kind in range(2):
            for k in range(2):
                for way in range(2):
                    self.message(self.slot(r), k, phase, kind, way).start()

    def middle(self, r, phase):
        slot = self.slot(r)
        for k in range(2):
            axis = k if phase == 0 else 1 - k
            for way in range(2):
                self.message(slot, k, phase, 0, way).wait_recv()
                mine = self.source(slot, k, phase, self.torus.step(axis, SIDES[way]), way)
                held = self.relay[phase].at[slot, k, way]
                held[...] = (held[...].astype(F32) + mine[...].astype(F32)).astype(BF)
                self.message(slot, k, phase, 2, way).start()

    def finish(self, r, phase):
        slot, q = self.slot(r), self.quarter
        for k in range(2):
            axis = k if phase == 0 else 1 - k
            for way in range(2):
                for kind in (1, 2):
                    self.message(slot, k, phase, kind, way).wait_recv()
            for half in range(2):
                mine = self.source(slot, k, phase, self.torus.step(axis, 0), half)
                side = self.side[phase]
                total = mine[...].astype(F32) + side[slot, k, 0, half].astype(F32) + side[slot, k, 1, half].astype(F32)
                if phase == 0:
                    self.partial[slot, k, :, :, :, pl.ds(half * q, q)] = total.astype(BF)
                else:
                    self.result(r, pl.ds((2 * k + half) * q, q), total.astype(BF))
            for way in range(2):
                for kind in (0, 1, 2):
                    self.message(slot, k, phase, kind, way).wait_send()

    def ways(self):
        return [(i, self.torus.device(a, b)) for i, (a, b) in enumerate((axis, side) for axis in range(2) for side in SIDES)]

    def give(self):
        for i, device in self.ways():
            pl.semaphore_signal(self.credit.at[i ^ 1], inc=1, device_id=device, device_id_type=MESH)

    def take(self):
        for i in range(4):
            pl.semaphore_wait(self.credit.at[i], 1)


LAG = 2
SLOTS = 5 * LAG


def step_kernel(layers, n, *refs):
    x_ref, dy_ref, gu_in, d_in, gu_ref, down_ref, grads_ref, down_grads_ref, squares_ref = refs[:9]
    hs_ref, a_ref, at_ref, by_ref, dag_ref, dau_ref, dg_ref, du_ref, act_ref, gub, downb, wsem, sq_ref, sq_all, sqs, sqr = refs[9:25]
    tokens, d = dy_ref.shape
    tiles, rows = grads_ref.shape[1], grads_ref.shape[3]
    per = n
    pairs = down_grads_ref.shape[2] // 2
    chunks, total_tiles = tiles // per, layers * tiles
    turns = per + pairs
    rounds = layers * chunks * turns
    torus = Torus(n)

    greet([torus.device(a, b) for a in range(2) for b in SIDES] + [torus.device(a, 2) for a in range(2)] + [partner_core()])

    start, stages, drain = gatherer(torus, 2 * layers, gu_in, d_in, gu_ref, down_ref, *refs[25:30])

    def enter(layer):
        wide = hs_ref[layer].astype(F32)
        wide = wide * scale_of(wide)
        a_ref[layer] = wide.astype(BF)
        at_ref[layer] = wide.T.astype(BF)

    def store(r, cols, total):
        chunk, turn = lax.div(r, turns), lax.rem(r, turns)
        layer, chunk = layers - 1 - lax.div(chunk, chunks), lax.rem(chunk, chunks)

        @pl.when(turn < per)
        def _():
            grads_ref[layer, chunk * per + turn, :, :, cols] = total

        @pl.when(turn >= per)
        def _():
            down_grads_ref[layer, chunk, pl.ds(2 * (turn - per), 2), :, cols] = total

        wide = total.astype(F32)
        sq_ref[...] += jnp.sum(wide * wide, axis=0)

    sums = Stream(torus, SLOTS, refs[30:], store)

    def fetch(layer, tile, buf):
        cols = pl.ds(pl.multiple_of(tile * TILE, TILE), TILE)
        return (
            pltpu.make_async_copy(gu_ref.at[layer, :, :, :, :, :, cols], gub.at[buf], wsem.at[buf, 0]),
            pltpu.make_async_copy(down_ref.at[layer, lax.div(tile, per), lax.rem(tile, per)], downb.at[buf], wsem.at[buf, 1]),
        )

    def begin(copies):
        for copy in copies:
            copy.start()

    def weights(buf):
        return gub[buf, 0].reshape(d, TILE), gub[buf, 1].reshape(d, TILE), downb[buf].reshape(TILE, d)

    def forward(layer):
        half, span = tokens // 2, tiles // 2
        dag_ref[...] = jnp.zeros_like(dag_ref)
        if layer > 0:
            begin(fetch(layer, 0, 0))

        def tile_step(i, _):
            s = i - span
            buf = lax.rem(i, 2)

            @pl.when(s >= 0)
            def _():
                for copy in fetch(layer, s, buf):
                    copy.wait()

            @pl.when((s + 1 >= 0) & (s + 1 < tiles))
            def _():
                begin(fetch(layer, s + 1, 1 - buf))

            @pl.when(s >= 0)
            def _():
                gate_w, up_w, down_w = weights(buf)
                for part in range(2):
                    these = pl.ds(part * half, half)
                    gate = dot(a_ref[layer, these, :], gate_w)
                    up = dot(a_ref[layer, these, :], up_w)
                    act = (gate * jax.nn.sigmoid(gate) * up).astype(BF)
                    dag_ref[these, :] += dot(act, down_w)

            for number, stage in enumerate(stages(2 * layer + lax.div(i, span))):
                pl.when(lax.rem(i, span) == number)(stage)
            return 0

        lax.fori_loop(span if layer > 0 else 0, span + tiles, tile_step, 0)
        hs_ref[layer + 1] = (hs_ref[layer].astype(F32) + dag_ref[...].astype(BF).astype(F32)).astype(BF)
        enter(layer + 1)

    def norm_back(layer):
        def block(i, _):
            these = pl.ds(pl.multiple_of(i * LANES, LANES), LANES)
            wide = hs_ref[layer, these, :].astype(F32)
            scale = scale_of(wide)
            da = (dag_ref[these, :].astype(BF).astype(F32) + dau_ref[these, :].astype(BF).astype(F32)).astype(BF).astype(F32)
            along = jnp.mean(da * wide, -1, keepdims=True)
            back = (da * scale - wide * (scale * scale * scale * along)).astype(BF)
            by_ref[these, :] = (by_ref[these, :].astype(F32) + back.astype(F32)).astype(BF)
            return 0

        lax.fori_loop(0, tokens // LANES, block, 0)

    def compute(r, layer):
        buf, t = lax.rem(r, 2), lax.rem(r, per)
        first = lax.div(r, per) * turns
        gate_w, up_w, down_w = weights(buf)
        half = tokens // 2
        for part in range(2):
            these = pl.ds(part * half, half)
            gate = dot(a_ref[layer, these, :], gate_w)
            up = dot(a_ref[layer, these, :], up_w)
            dact = dot(by_ref[these, :], down_w, (1, 1)).astype(BF).astype(F32)
            sig = jax.nn.sigmoid(gate)
            silu = gate * sig
            act_ref[these, :] = (silu * up).astype(BF)
            du_ref[these, :] = (dact * silu).astype(BF)
            dg_ref[these, :] = (dact * up * (sig * (1.0 + gate * (1.0 - sig)))).astype(BF)
        for which, ref in enumerate((dg_ref, du_ref)):
            sums.staged[sums.slot(first + t), which] = dot(at_ref[layer], ref[...]).astype(BF).reshape(n, n, rows, TILE)
        by_down = dot(act_ref[...], by_ref[...], (0, 0)).astype(BF).reshape(n, 2 * pairs, rows, d)
        for m in range(2 * pairs):
            sums.staged[sums.slot(first + per + m // 2), m % 2, t] = by_down[:, m]

        @pl.when(layer > 0)
        def _():
            dag_ref[...] += dot(dg_ref[...], gate_w, (1, 1))
            dau_ref[...] += dot(du_ref[...], up_w, (1, 1))

    def turn(r, _):
        @pl.when(r < rounds)
        def _():
            @pl.when(r >= SLOTS)
            def _():
                sums.take()

            sums.issue(r, 0)

        def late(stages):
            return (r >= stages * LAG) & (r < rounds + stages * LAG)

        @pl.when(late(1))
        def _():
            sums.middle(r - LAG, 0)

        @pl.when(late(2))
        def _():
            sums.finish(r - 2 * LAG, 0)
            sums.issue(r - 2 * LAG, 1)

        @pl.when(late(3))
        def _():
            sums.middle(r - 3 * LAG, 1)

        @pl.when(late(4))
        def _():
            sums.finish(r - 4 * LAG, 1)

            @pl.when(r - 4 * LAG + SLOTS < rounds)
            def _():
                sums.give()

        return 0

    sq_ref[...] = jnp.zeros_like(sq_ref)
    by_ref[...] = dy_ref[...]
    start()
    hs_ref[0] = x_ref[...]
    enter(0)
    for layer in range(layers - 1):
        forward(layer)
    begin(fetch(layers - 1, 0, 0))

    def tile_step(r, _):
        t, first = lax.rem(r, per), lax.div(r, per) * turns

        for number, stage in enumerate(stages(2 * layers - 1)):
            pl.when(r == number // 2)(stage)

        @pl.when(r < total_tiles)
        def _():
            layer = layers - 1 - lax.div(r, tiles)
            for copy in fetch(layer, lax.rem(r, tiles), lax.rem(r, 2)):
                copy.wait()

            @pl.when(r + 1 < total_tiles)
            def _():
                begin(fetch(layers - 1 - lax.div(r + 1, tiles), lax.rem(r + 1, tiles), 1 - lax.rem(r, 2)))

            @pl.when(lax.rem(r, tiles) == 0)
            def _():
                @pl.when(r > 0)
                def _():
                    norm_back(layer + 1)

                dag_ref[...] = jnp.zeros_like(dag_ref)
                dau_ref[...] = jnp.zeros_like(dau_ref)

            compute(r, layer)

        more = 1 + pairs * lax.div(t + 1, per) + (4 * LAG - 1) * lax.div(r, total_tiles)
        lax.fori_loop(first + t, first + t + more, turn, 0)
        return 0

    lax.fori_loop(0, total_tiles + 1, tile_step, 0)
    drain()

    mine = jnp.sum(sq_ref[...], axis=0, keepdims=True)
    sq_all[0, 0] = jnp.broadcast_to(mine, sq_all.shape[2:])
    for axis in range(2):
        copies = [
            pltpu.make_async_remote_copy(
                sq_all.at[axis, 0], sq_all.at[axis, 1 + i], sqs.at[axis, i], sqr.at[axis, i], device_id=torus.device(axis, by), device_id_type=MESH
            )
            for i, by in enumerate((1, 2, -1))
        ]
        for copy in copies:
            copy.start()
        for copy in copies:
            copy.wait()
        total = sum(sq_all[axis, i] for i in range(1, n)) + sq_all[axis, 0]
        if axis == 0:
            sq_all[1, 0] = total
        else:
            squares_ref[...] = total


def gradients(x, dy, gu, down, n):
    layers, chunks, (tokens, d), ff = gu.shape[0], down.shape[1], x.shape, gu.shape[-1]
    rows, quarter, tiles = d // (n * n), TILE // 4, ff // TILE
    vmem, anywhere = pl.BlockSpec(memory_space=pltpu.VMEM), pl.BlockSpec(memory_space=pl.ANY)
    dma = pltpu.SemaphoreType.DMA

    both, block = (SLOTS, 2, 2), (2, n, rows, quarter)
    stream = [
        pltpu.VMEM((SLOTS, 2, n, n, rows, TILE), BF),
        pltpu.VMEM(both + block, BF),
        pltpu.VMEM(both + (2,) + block, BF),
        pltpu.VMEM((SLOTS, 2, 2, n, rows, 2 * quarter), BF),
        pltpu.VMEM(both + (2, rows, quarter), BF),
        pltpu.VMEM(both + (2, 2, rows, quarter), BF),
        dma(both + (3, 2)),
        dma(both + (3, 2)),
        pltpu.SemaphoreType.REGULAR((4,)),
    ]

    return pl.pallas_call(
        functools.partial(step_kernel, layers, n),
        out_shape=(
            jax.ShapeDtypeStruct((layers, 2, n, n) + gu.shape[2:], BF),
            jax.ShapeDtypeStruct((layers, chunks, n, n) + down.shape[2:], BF),
            jax.ShapeDtypeStruct((layers, tiles, 2, rows, TILE), BF),
            jax.ShapeDtypeStruct((layers, chunks, LANES // rows, rows, d), BF),
            jax.ShapeDtypeStruct((8, LANES), F32),
        ),
        in_specs=[vmem] * 4,
        out_specs=(anywhere, anywhere, vmem, vmem, vmem),
        scratch_shapes=[
            pltpu.VMEM((layers, tokens, d), BF),
            pltpu.VMEM((layers, tokens, d), BF),
            pltpu.VMEM((layers, d, tokens), BF),
            pltpu.VMEM((tokens, d), BF),
            pltpu.VMEM((tokens, d), F32),
            pltpu.VMEM((tokens, d), F32),
            pltpu.VMEM((tokens, TILE), BF),
            pltpu.VMEM((tokens, TILE), BF),
            pltpu.VMEM((tokens, TILE), BF),
            pltpu.VMEM((2, 2, n, n) + gu.shape[2:-1] + (TILE,), BF),
            pltpu.VMEM((2, n) + down.shape[2:], BF),
            dma((2, 2)),
            pltpu.VMEM((rows, quarter), F32),
            pltpu.VMEM((2, n, 8, LANES), F32),
            dma((2, n - 1)),
            dma((2, n - 1)),
            dma((2 * layers, 2, 5, 4, 2)),
            dma((2 * layers, 2, 5, 4, 2)),
            dma((2 * layers, 2, 15, 2)),
            dma((2 * layers, 2, 15, 2)),
            dma((layers, 2)),
        ]
        + stream,
        compiler_params=pltpu.CompilerParams(collective_id=0, has_side_effects=True, vmem_limit_bytes=VMEM_LIMIT),
        cost_estimate=pl.CostEstimate(flops=34 * tokens * d * ff, bytes_accessed=18 * d * ff, transcendentals=3 * tokens * ff),
    )(x, dy, gu, down)


def update_kernel(count, n, grads_ref, down_grads_ref, squares_ref, *refs):
    w, m, v, new_w, new_m, new_v = (refs[i : i + 3] for i in range(0, 18, 3))
    squares = jnp.sum(squares_ref[0:1, :], axis=1, keepdims=True)
    factor = jnp.minimum(1.0, 0.5 * lax.rsqrt(squares / count + 1e-30))

    def put(which, at, g):
        new = adamw(w[which][at].astype(F32), m[which][at], v[which][at], g.astype(F32) * factor)
        for ref, value in zip((new_w[which], new_m[which], new_v[which]), new, strict=True):
            ref[at] = value

    t = pl.program_id(1)
    rows, span = w[0].shape[1:]
    for which in range(2):
        for y in range(n):
            for q in range(span // (n * LANES)):
                at = (0, slice(None), pl.ds((y * (span // (n * LANES)) + q) * LANES, LANES))
                put(which, at, grads_ref[0, q * n + t, which, :, pl.ds(y * LANES, LANES)])
    for i in range(down_grads_ref.shape[2]):
        put(2, (0, pl.ds(i * rows, rows)), down_grads_ref[0, 0, i])


def update(grads, down_grads, squares, weights, m, v, n, count):
    layers, rows, ff = weights[0].shape
    tall, d = weights[2].shape[1:]
    steps = n
    wide = pl.BlockSpec((1, rows, ff // steps), lambda l, t: (l, 0, t))
    high = pl.BlockSpec((1, tall // steps, d), lambda l, t: (l, t, 0))
    three = [wide, wide, high]
    shapes = [jax.ShapeDtypeStruct(w.shape, kind) for kind in (BF, F32, F32) for w in weights]
    return pl.pallas_call(
        functools.partial(update_kernel, count, n),
        grid=(layers, steps),
        out_shape=tuple(shapes),
        in_specs=[
            pl.BlockSpec((1,) + grads.shape[1:], lambda l, t: (l, 0, 0, 0, 0)),
            pl.BlockSpec((1, 1) + down_grads.shape[2:], lambda l, t: (l, t, 0, 0, 0)),
            pl.BlockSpec(squares.shape, lambda l, t: (0, 0)),
        ]
        + three * 3,
        out_specs=tuple(three * 3),
        compiler_params=pltpu.CompilerParams(vmem_limit_bytes=VMEM_LIMIT),
    )(grads, down_grads, squares, *weights, *m, *v)


def solution(mesh):
    group = mesh.shape["dp"]
    n = math.isqrt(group)
    assert n == 4 and n * n == group

    def step(x, dy, *arrays):
        weights, m, v = (arrays[i : i + 3] for i in (0, 3, 6))
        layers, rows, ff = weights[0].shape
        d = weights[2].shape[-1]
        tall = ff // group
        chunks = tall // LANES
        gu = jnp.stack([w.reshape(layers, rows, group, chunks, LANES).swapaxes(2, 3).reshape(layers, rows, ff) for w in weights[:2]], axis=1)
        gu, down = gu.reshape(layers, 2, 2, rows // 2, ff), weights[2].reshape(layers, chunks, LANES, d)
        _, _, grads, down_grads, squares = gradients(x[0], dy[0], gu, down, n)
        return update(grads, down_grads, squares, weights, m, v, n, group * sum(w.size for w in weights))

    states, cut = P(("rep", "dp"), None, None), P(None, "dp", None)
    return jax.shard_map(
        step,
        mesh=mesh,
        in_specs=(states, states) + (cut,) * 9,
        out_specs=(P("rep", "dp", None),) * 9,
        check_vma=False,
    )
```
